16 devices in a mesh: dp: 2 (over z), sp: 8 (over y, x, core).
Axes of the slice: x: 2, y: 2, z: 2, core: 2. Of those that a mesh axis runs over, the one named last changes fastest.
Arguments:
- x: bfloat16 [4, 4096], P('dp'), parts along dimension 0
- wq: bfloat16 [4096, 4096], replicated
- wk: bfloat16 [4096, 1024], replicated
- wv: bfloat16 [4096, 1024], replicated
- wo: bfloat16 [4096, 4096], P('sp')
- kc: bfloat16 [4, 32768, 8, 128], P('dp', 'sp'), parts along dimension 0
- vc: bfloat16 [4, 32768, 8, 128], P('dp', 'sp'), parts along dimension 0
- pos: int32 [4], P('dp'), parts along dimension 0
- lens: int32 [4], P('dp'), parts along dimension 0
Outputs:
- output 1: bfloat16 [4, 4096], P('dp'), parts along dimension 0
- output 2: bfloat16 [4, 32768, 8, 128], P('dp', 'sp'), parts along dimension 0
- output 3: bfloat16 [4, 32768, 8, 128], P('dp', 'sp'), parts along dimension 0
There are 2 independent parts. The reference program is written for one: setup_inputs(seed, part) draws one part's arguments, and reference() takes and returns one part's arrays. A program takes and returns all parts, laid end to end along the dimension named above; an argument that names none is the same for every part.
All inputs are finite; a program needn't handle non-finite values.
Results may differ from the reference program's by a relative error of at most 0.00351591.
Values are sent between devices in bfloat16 or wider.
A program may use at most 1 GiB of HBM per device.

```python
import math
import jax
import jax.numpy as jnp
from jax import lax

B = 2
S = 32768
D = 4096
HEADS = 32
KV_HEADS = 8
HEAD = 128

G = HEADS // KV_HEADS
RCH = min(S, 2048)


def _cache(key, phase, noise):
    ka, kn = jax.random.split(key)
    nf = phase.shape[0]
    amp = jax.random.normal(ka, (B, KV_HEADS, nf, HEAD), jnp.float32) * (2.0 / nf) ** 0.5
    freq = jnp.arange(1, nf + 1).astype(jnp.float32)
    nc = S // RCH

    def piece(i):
        t = ((i % nc) * RCH + jnp.arange(RCH)).astype(jnp.float32) / S
        phi = jnp.cos(2.0 * math.pi * freq[None, :] * t[:, None] + phase[None, :])
        smooth = jnp.einsum('tf,kfd->tkd', phi, amp[i // nc])
        z = jax.random.normal(jax.random.fold_in(kn, i), (RCH, KV_HEADS, HEAD), jnp.float32)
        return (smooth + noise * z).astype(jnp.bfloat16)

    return lax.map(piece, jnp.arange(B * nc)).reshape(B, S, KV_HEADS, HEAD)


def setup_inputs(seed: int = 0, part: int = 0) -> dict:
    ks = jax.random.split(jax.random.PRNGKey(seed), 12)
    pk = [jax.random.fold_in(k, part) for k in ks[5:]]
    u = jax.random.normal(ks[0], (D, KV_HEADS, 1, HEAD), jnp.float32)
    wq = (u + jax.random.normal(ks[1], (D, KV_HEADS, G, HEAD), jnp.float32)) * (2.0 * D) ** -0.5
    gamma = math.log(0.1 * S) * (2.0 / HEAD) ** 0.5
    wk = (gamma * u[:, :, 0] + 0.5 * jax.random.normal(ks[2], (D, KV_HEADS, HEAD), jnp.float32)) * D ** -0.5
    wv = jax.random.normal(ks[3], (D, KV_HEADS * HEAD), jnp.float32) * D ** -0.5
    wo = jax.random.normal(ks[4], (HEADS * HEAD, D), jnp.float32) * (HEADS * HEAD) ** -0.5
    x = jax.random.normal(pk[0], (B, D), jnp.float32)
    lens = jax.random.randint(pk[1], (B,), S // 32, S + 1, jnp.int32)
    kc = _cache(pk[2], jax.random.uniform(pk[3], (4,), jnp.float32, 0.0, 2.0 * math.pi), 0.6)
    vc = _cache(pk[4], jax.random.uniform(pk[5], (4,), jnp.float32, 0.0, 2.0 * math.pi), 0.5)
    return {
        'x': x.astype(jnp.bfloat16),
        'wq': wq.reshape(D, HEADS * HEAD).astype(jnp.bfloat16),
        'wk': wk.reshape(D, KV_HEADS * HEAD).astype(jnp.bfloat16),
        'wv': wv.astype(jnp.bfloat16),
        'wo': wo.astype(jnp.bfloat16),
        'kc': kc,
        'vc': vc,
        'pos': lens - 1,
        'lens': lens,
    }


def reference(x, wq, wk, wv, wo, kc, vc, pos, lens):
    q = jnp.dot(x, wq, preferred_element_type=jnp.float32).astype(jnp.bfloat16).reshape(B, KV_HEADS, G, HEAD)
    k = jnp.dot(x, wk, preferred_element_type=jnp.float32).astype(jnp.bfloat16).reshape(B, KV_HEADS, HEAD)
    v = jnp.dot(x, wv, preferred_element_type=jnp.float32).astype(jnp.bfloat16).reshape(B, KV_HEADS, HEAD)
    bi = jnp.arange(B)
    kn = kc.at[bi, pos].set(k)
    vn = vc.at[bi, pos].set(v)
    qf = q.astype(jnp.float32)

    def block(c):
        kb = lax.dynamic_slice_in_dim(kn, c * RCH, RCH, axis=1).astype(jnp.float32)
        vb = lax.dynamic_slice_in_dim(vn, c * RCH, RCH, axis=1).astype(jnp.float32)
        s = jnp.einsum('bkgd,bskd->bkgs', qf, kb) * HEAD ** -0.5
        valid = (c * RCH + jnp.arange(RCH))[None, :] < lens[:, None]
        s = jnp.where(valid[:, None, None, :], s, -jnp.inf)
        m = s.max(-1)
        p = jnp.exp(s - jnp.where(jnp.isfinite(m), m, 0.0)[..., None])
        return m, p.sum(-1), jnp.einsum('bkgs,bskd->bkgd', p, vb)

    m, l, o = lax.map(block, jnp.arange(S // RCH))
    a = jnp.exp(m - m.max(0))
    out = (a[..., None] * o).sum(0) / (a * l).sum(0)[..., None]
    out = out.astype(jnp.bfloat16).reshape(B, HEADS * HEAD)
    y = jnp.dot(out, wo, preferred_element_type=jnp.float32).astype(jnp.bfloat16)
    return (y, kn, vn)
```

```python
import functools

import jax
import jax.numpy as jnp
from jax import lax
from jax.experimental import pallas as pl
from jax.experimental.pallas import tpu as pltpu
from jax.sharding import PartitionSpec as P

MESH = pl.DeviceIdType.MESH
ANY = pl.BlockSpec(memory_space=pl.ANY)
VMEM = pl.BlockSpec(memory_space=pltpu.VMEM)
SMEM = pl.BlockSpec(memory_space=pltpu.SMEM)
f32 = jnp.float32
bf16 = jnp.bfloat16
LOG2E = 1.4426950408889634
MIB = 1 << 20


def greet(n):
    me = lax.axis_index('sp')
    barrier = pltpu.get_barrier_semaphore()
    for d in range(1, n):
        pl.semaphore_signal(barrier, inc=1, device_id={'sp': lax.rem(me + d, n)}, device_id_type=MESH)


def awaited(n):
    pl.semaphore_wait(pltpu.get_barrier_semaphore(), n - 1)


def lookup(n, wch, ch, slabs, early, pos, lens, x, wq, wk, wv, kc, vc, gat_out, kbuf, vbuf, sc, mrun, snew,
           xb, wqb, wkb, wvb, send, gat, qbd, xsem, wsem, ksem, vsem, ssem, rsem):
    me = lax.axis_index('sp')
    nb, dm = xb.shape
    dq, dh = wqb.shape[1], wkb.shape[1]
    rows = dm // wch
    g = dq // dh
    nkv = n
    npos = kbuf.shape[1] // nkv
    nch = npos // ch
    total = nb * nch
    crow = ch * nkv
    srow = crow // slabs
    heads = 128 // slabs
    start = me * npos
    ninf = -jnp.inf

    def chunk(i):
        return i // nch, pl.ds(pl.multiple_of(i % nch * crow, crow), crow)

    def read_k(i):
        b, r = chunk(i)
        return pltpu.make_async_copy(kc.at[b, r], kbuf.at[b, r], ksem.at[i])

    def read_v(i):
        b, r = chunk(i)
        return pltpu.make_async_copy(vc.at[b, r], vbuf.at[b, r], vsem.at[i])

    xcp = pltpu.make_async_copy(x, xb, xsem)
    xcp.start()
    cps = []
    for c in range(wch):
        r = pl.ds(c * rows, rows)
        trio = []
        for j, (w, buf, cols) in enumerate(((wq, wqb, dq), (wk, wkb, dh), (wv, wvb, dh))):
            cp = pltpu.make_async_copy(w.at[r, pl.ds(pl.multiple_of(me * cols, 128), cols)], buf.at[r], wsem.at[j, c])
            cp.start()
            trio.append(cp)
        cps.append(trio)
    greet(n)
    xcp.wait()
    aq = jnp.zeros((nb, dq), f32)
    ak = jnp.zeros((nb, dh), f32)
    av = jnp.zeros((nb, dh), f32)
    for c in range(wch):
        for cp in cps[c]:
            cp.wait()
        for i in range(c * total // wch, (c + 1) * total // wch):
            read_k(i).start()
        xc = xb[:, c * rows:(c + 1) * rows]
        r = pl.ds(c * rows, rows)
        aq += jnp.dot(xc, wqb[r, :], preferred_element_type=f32)
        ak += jnp.dot(xc, wkb[r, :], preferred_element_type=f32)
        av += jnp.dot(xc, wvb[r, :], preferred_element_type=f32)
    for b in range(nb):
        pieces = [aq[b:b + 1, i * dh:(i + 1) * dh] for i in range(g)] + [ak[b:b + 1], av[b:b + 1]]
        pieces.append(jnp.zeros((8 - g - 2, dh), f32))
        tile = jnp.concatenate(pieces, axis=0).astype(bf16)
        send[b] = tile
        gat[me, b] = tile
    for i in range(early):
        read_v(i).start()
    awaited(n)
    out = []
    for d in range(1, n):
        cp = pltpu.make_async_remote_copy(
            src_ref=send, dst_ref=gat.at[me], send_sem=ssem.at[d], recv_sem=rsem.at[d],
            device_id={'sp': lax.rem(me + d, n)}, device_id_type=MESH)
        cp.start()
        out.append(cp)
    for cp in out:
        cp.wait()

    gat_out[...] = gat[...]
    gf = gat[...].astype(f32)
    sub = lax.broadcasted_iota(jnp.int32, (nkv, 128), 0)
    lane = lax.broadcasted_iota(jnp.int32, (nkv, 128), 1)
    own = sub == (lane % heads) // g
    first = jnp.where(own, lane // heads * (ch // slabs), 1 << 29)
    for b in range(nb):
        q = jnp.concatenate([gf[i, b, 0:g] for i in range(nkv)], axis=0)
        kn = jnp.concatenate([gf[i, b, g:g + 1] for i in range(nkv)], axis=0)
        zero = jnp.zeros_like(q)
        for s in range(slabs):
            a = jnp.concatenate([q if i == s else zero for i in range(slabs)], axis=0)
            qbd[b, s * dh:(s + 1) * dh, :] = a.T.astype(bf16)
        k16 = jnp.concatenate([kn, jnp.zeros_like(kn)], axis=0).astype(bf16)
        t = jnp.dot(k16, qbd[b, 0:dh, :], preferred_element_type=f32)[0:nkv]
        here = jnp.logical_and(pos[b] >= start, pos[b] < jnp.minimum(start + npos, lens[b]))
        limit = jnp.where(here, heads, 0)
        t = jnp.where(jnp.logical_and(own, lane < limit), t, ninf)
        snew[b] = t
        mrun[b] = t

    def scores(i, _):
        b, c = i // nch, i % nch
        read_k(i).wait()

        @pl.when(i + early < total)
        def _():
            read_v(i + early).start()

        lim = jnp.minimum(pos[b], lens[b]) - start - c * ch
        acc = None
        for s in range(0, slabs, 2):
            k2 = jnp.concatenate(
                [kbuf[b, pl.ds(pl.multiple_of(c * crow + (s + t) * srow, srow), srow), :] for t in range(2)], axis=1)
            t = jnp.dot(k2, qbd[b, s * dh:(s + 2) * dh, :], preferred_element_type=f32)
            acc = t if acc is None else acc + t
        acc = acc.reshape(srow // nkv, nkv, 128)
        left = lim - lax.broadcasted_iota(jnp.int32, acc.shape, 0)
        t = jnp.where(first[None] < left, acc, ninf)
        sc[b, pl.ds(pl.multiple_of(c * srow, srow), srow), :] = t.reshape(srow, 128)
        mrun[b] = jnp.maximum(mrun[b], t.max(0))
        return 0

    lax.fori_loop(0, total, scores, 0)

    def landed(i, _):
        read_v(i).wait()
        return 0

    lax.fori_loop(0, total, landed, 0)


def attend(ch, slabs, pos, lens, gat, kbuf, vbuf, sc, mrun, snew, part, ko, vo, mall, lrun, orun, knew, vnew,
           ksem, vsem, nsem):
    me = lax.axis_index('sp')
    nkv, nb, _, dh = gat.shape
    npos = kbuf.shape[1] // nkv
    nch = npos // ch
    total = nb * nch
    crow = ch * nkv
    srow = crow // slabs
    heads = 128 // slabs
    g = heads // nkv
    start = me * npos
    scale = dh ** -0.5 * LOG2E
    ninf = -jnp.inf

    def writes(i):
        b, r = i // nch, pl.ds(pl.multiple_of(i % nch * crow, crow), crow)
        return (pltpu.make_async_copy(kbuf.at[b, r], ko.at[b, r], ksem.at[i]),
                pltpu.make_async_copy(vbuf.at[b, r], vo.at[b, r], vsem.at[i]))

    def begin(i, _):
        for cp in writes(i):
            cp.start()
        return 0

    lax.fori_loop(0, total, begin, 0)

    gf = gat[...].astype(f32)
    lrun[...] = jnp.zeros_like(lrun)
    orun[...] = jnp.zeros_like(orun)
    for b in range(nb):
        knew[b] = jnp.concatenate([gf[i, b, g:g + 1] for i in range(nkv)], axis=0).astype(bf16)
        vnew[b] = jnp.concatenate([gf[i, b, g + 1:g + 2] for i in range(nkv)], axis=0).astype(bf16)
        m = jnp.broadcast_to(mrun[b].max(0, keepdims=True), (nkv, 128))
        k = heads
        while k < 128:
            m = jnp.maximum(m, pltpu.roll(m, k, 1))
            k *= 2
        mall[b] = m

    def mix(i, _):
        b, c = i // nch, i % nch
        lim = jnp.minimum(pos[b], lens[b]) - start - c * ch

        @pl.when(lim > 0)
        def _():
            m = mall[b]
            m = jnp.where(m == ninf, 0.0, m)
            t = sc[b, pl.ds(pl.multiple_of(c * srow, srow), srow), :].reshape(srow // nkv, nkv, 128)
            e = jnp.exp2((t - m[None]) * scale)
            lrun[b] += e.sum(0)
            et = e.reshape(srow, 128).astype(bf16).T
            o = orun[b]
            for s in range(slabs):
                v = vbuf[b, pl.ds(pl.multiple_of(c * crow + s * srow, srow), srow), :]
                o += jnp.dot(et[s * heads:(s + 1) * heads], v, preferred_element_type=f32)
            orun[b] = o

        return 0

    lax.fori_loop(0, total, mix, 0)

    half = lax.broadcasted_iota(jnp.int32, (heads, 128), 1) < 64
    for b in range(nb):
        m = mall[b]
        e = jnp.exp2((snew[b] - jnp.where(m == ninf, 0.0, m)) * scale)
        pad = jnp.zeros_like(e)
        e16 = jnp.concatenate([e, pad], axis=0).astype(bf16)
        v16 = jnp.concatenate([vnew[b].astype(f32), pad], axis=0).astype(bf16)
        o = orun[b] + lax.dot_general(e16, v16, (((0,), (0,)), ((), ())), preferred_element_type=f32)[0:heads]
        l = jnp.broadcast_to((lrun[b] + e).sum(0, keepdims=True), (nkv, 128))
        k = heads
        while k < 128:
            l = l + pltpu.roll(l, k, 1)
            k *= 2
        lt = jnp.broadcast_to(l[0:1], (128, 128)).T[0:heads]
        mt = jnp.broadcast_to(m[0:1] * scale, (128, 128)).T[0:heads]
        ml = jnp.where(half, mt, lt)
        for i in range(nkv):
            part[i, 0, b * g:(b + 1) * g, :] = o[i * g:(i + 1) * g, :]
            part[i, 1, b * g:(b + 1) * g, :] = ml[i * g:(i + 1) * g, :]

    def written(i, _):
        for cp in writes(i):
            cp.wait()
        return 0

    lax.fori_loop(0, total, written, 0)
    for b in range(nb):
        p = pos[b] - start

        @pl.when(jnp.logical_and(p >= 0, p < npos))
        def _():
            r = pl.ds(pl.multiple_of(p * nkv, nkv), nkv)
            cps = (pltpu.make_async_copy(knew.at[b], ko.at[b, r], nsem.at[0]),
                   pltpu.make_async_copy(vnew.at[b], vo.at[b, r], nsem.at[1]))
            for cp in cps:
                cp.start()
            for cp in cps:
                cp.wait()


def combine(n, nb, ych, part, wo, y, wob, rbuf, xs, ybuf, wsem, ssem, rsem, ysem, zsem):
    me = lax.axis_index('sp')
    cols = wo.shape[1] // ych
    cps = []
    for c in range(ych):
        cp = pltpu.make_async_copy(wo.at[:, pl.ds(c * cols, cols)], wob.at[c], wsem.at[c])
        cp.start()
        cps.append(cp)
    greet(n)
    awaited(n)
    out = []
    for d in range(1, n):
        peer = lax.rem(me + d, n)
        cp = pltpu.make_async_remote_copy(
            src_ref=part.at[peer], dst_ref=rbuf.at[me], send_sem=ssem.at[d], recv_sem=rsem.at[d],
            device_id={'sp': peer}, device_id_type=MESH)
        cp.start()
        out.append(cp)
    rbuf[me] = part[me]
    for cp in out:
        cp.wait()
    o = rbuf[:, 0]
    ml = rbuf[:, 1]
    m = jnp.broadcast_to(ml[:, :, 0:1], o.shape)
    l = jnp.broadcast_to(ml[:, :, 64:65], o.shape)
    a = jnp.exp2(m - m.max(0)[None])
    out8 = (a * o).sum(0) / (a * l).sum(0)
    g = out8.shape[0] // nb
    dh = out8.shape[1]
    xs[...] = jnp.zeros_like(xs)
    for b in range(nb):
        for j in range(g):
            xs[b:b + 1, j * dh:(j + 1) * dh] = out8[b * g + j:b * g + j + 1]
    xl = xs[...].astype(bf16)
    sent = []
    for c in range(ych):
        cps[c].wait()
        ybuf[me, c] = jnp.dot(xl, wob[c], preferred_element_type=f32)[0:nb]
        for d in range(1, n):
            cp = pltpu.make_async_remote_copy(
                src_ref=ybuf.at[me, c], dst_ref=ybuf.at[me, c], send_sem=ysem.at[c, d], recv_sem=zsem.at[c, d],
                device_id={'sp': lax.rem(me + d, n)}, device_id_type=MESH)
            cp.start()
            sent.append(cp)
    for cp in sent:
        cp.wait()
    for c in range(ych):
        t = ybuf[0, c]
        for i in range(1, n):
            t = t + ybuf[i, c]
        y[:, c * cols:(c + 1) * cols] = t.astype(bf16)


def solution(mesh):
    n = mesh.shape['sp']

    def local(x, wq, wk, wv, wo, kc, vc, pos, lens):
        nb, npos, nkv, dh = kc.shape
        dm = x.shape[1]
        dq = wq.shape[1] // n
        dma = pltpu.SemaphoreType.DMA
        kc = kc.reshape(nb, npos * nkv, dh)
        vc = vc.reshape(nb, npos * nkv, dh)
        wch, ch, slabs, early = 8, 512, 4, 8
        nch = npos // ch
        small = jax.ShapeDtypeStruct((nb, nkv, 128), f32)
        gat, kbuf, vbuf, sc, mrun, snew = pl.pallas_call(
            functools.partial(lookup, n, wch, ch, slabs, early),
            name='lookup',
            out_shape=(jax.ShapeDtypeStruct((n, nb, 8, dh), bf16), pltpu.VMEM(kc.shape, bf16), pltpu.VMEM(vc.shape, bf16),
                       pltpu.VMEM((nb, npos * nkv // slabs, 128), f32), small, small),
            in_specs=[SMEM, SMEM] + [ANY] * 6,
            out_specs=(VMEM,) * 6,
            scratch_shapes=[
                pltpu.VMEM(x.shape, bf16), pltpu.VMEM((dm, dq), bf16), pltpu.VMEM((dm, dh), bf16), pltpu.VMEM((dm, dh), bf16),
                pltpu.VMEM((nb, 8, dh), bf16), pltpu.VMEM((n, nb, 8, dh), bf16), pltpu.VMEM((nb, slabs * dh, 128), bf16),
                dma, dma((3, wch)), dma((nb * nch,)), dma((nb * nch,)), dma((n,)), dma((n,))],
            compiler_params=pltpu.CompilerParams(collective_id=0, has_side_effects=True, vmem_limit_bytes=12 * MIB),
        )(pos, lens, *(pltpu.with_memory_space_constraint(t, pltpu.HBM) for t in (x, wq, wk, wv, kc, vc)))

        part, ko, vo = pl.pallas_call(
            functools.partial(attend, ch, slabs),
            name='attend',
            out_shape=(jax.ShapeDtypeStruct((n, 2, 8, dh), f32), pltpu.HBM(kc.shape, bf16), pltpu.HBM(vc.shape, bf16)),
            in_specs=[SMEM, SMEM] + [VMEM] * 6,
            out_specs=(VMEM, ANY, ANY),
            scratch_shapes=[
                pltpu.VMEM((nb, nkv, 128), f32), pltpu.VMEM((nb, nkv, 128), f32), pltpu.VMEM((nb, 128 // slabs, dh), f32),
                pltpu.VMEM((nb, nkv, dh), bf16), pltpu.VMEM((nb, nkv, dh), bf16),
                dma((nb * nch,)), dma((nb * nch,)), dma((2,))],
            compiler_params=pltpu.CompilerParams(vmem_limit_bytes=12 * MIB),
        )(pos, lens, gat, kbuf, vbuf, sc, mrun, snew)

        ych = 4
        cols = wo.shape[1] // ych
        y = pl.pallas_call(
            functools.partial(combine, n, nb, ych),
            name='combine',
            out_shape=jax.ShapeDtypeStruct((nb, wo.shape[1]), bf16),
            in_specs=[VMEM, ANY],
            out_specs=VMEM,
            scratch_shapes=[
                pltpu.VMEM((ych, wo.shape[0], cols), bf16), pltpu.VMEM((n, 2, 8, dh), f32), pltpu.VMEM((8, wo.shape[0]), f32),
                pltpu.VMEM((n, ych, nb, cols), f32),
                dma((ych,)), dma((n,)), dma((n,)), dma((ych, n)), dma((ych, n))],
            compiler_params=pltpu.CompilerParams(collective_id=1, has_side_effects=True, vmem_limit_bytes=8 * MIB),
        )(part, pltpu.with_memory_space_constraint(wo, pltpu.HBM))
        shape = (nb, npos, nkv, dh)
        return y, ko.reshape(shape), vo.reshape(shape)

    cache = P('dp', 'sp', None, None)
    return jax.shard_map(
        local, mesh=mesh,
        in_specs=(P('dp', None), P(None, None), P(None, None), P(None, None), P('sp', None),
                  cache, cache, P('dp'), P('dp')),
        out_specs=(P('dp', None), cache, cache),
        check_vma=False)
```

```python
import functools

import jax
import jax.numpy as jnp
from jax import lax
from jax.experimental import pallas as pl
from jax.experimental.pallas import tpu as pltpu
from jax.sharding import PartitionSpec as P

MESH = pl.DeviceIdType.MESH
ANY = pl.BlockSpec(memory_space=pl.ANY)
VMEM = pl.BlockSpec(memory_space=pltpu.VMEM)
SMEM = pl.BlockSpec(memory_space=pltpu.SMEM)
f32 = jnp.float32
bf16 = jnp.bfloat16
LOG2E = 1.4426950408889634
MIB = 1 << 20


def greet(n):
    me = lax.axis_index('sp')
    barrier = pltpu.get_barrier_semaphore()
    for d in range(1, n):
        pl.semaphore_signal(barrier, inc=1, device_id={'sp': lax.rem(me + d, n)}, device_id_type=MESH)


def awaited(n):
    pl.semaphore_wait(pltpu.get_barrier_semaphore(), n - 1)


def lookup(n, wch, ch, wide, slabs, early, pos_hbm, lens_hbm, x, wq, wk, wv, kc, vc, gat_out, kbuf, vbuf, sc, mrun, snew,
           pos, lens, xb, wqb, wkb, wvb, send, gat, qbd, isem, xsem, wsem, ksem, vsem, ssem, rsem):
    me = lax.axis_index('sp')
    nb, dm = xb.shape
    dq, dh = wqb.shape[1], wkb.shape[1]
    rows = dm // wch
    g = dq // dh
    nkv = n
    npos = kbuf.shape[1] // nkv
    nch = npos // ch
    total = nb * nch
    crow = ch * nkv
    srow = crow // slabs
    heads = 128 // slabs
    start = me * npos
    ninf = -jnp.inf

    def chunk(i):
        return i // nch, pl.ds(pl.multiple_of(i % nch * crow, crow), crow)

    def read_k(i):
        b, r = chunk(i)
        return pltpu.make_async_copy(kc.at[b, r], kbuf.at[b, r], ksem.at[i])

    def read_v(i):
        b, r = chunk(i)
        return pltpu.make_async_copy(vc.at[b, r], vbuf.at[b, r], vsem.at[i])

    xcp = pltpu.make_async_copy(x, xb, xsem)
    xcp.start()
    icps = [pltpu.make_async_copy(pos_hbm, pos, isem.at[0]), pltpu.make_async_copy(lens_hbm, lens, isem.at[1])]
    for cp in icps:
        cp.start()
    cps = []
    for c in range(wch):
        r = pl.ds(c * rows, rows)
        trio = []
        for j, (w, buf, cols) in enumerate(((wq, wqb, dq), (wk, wkb, dh), (wv, wvb, dh))):
            cp = pltpu.make_async_copy(w.at[r, pl.ds(pl.multiple_of(me * cols, 128), cols)], buf.at[r], wsem.at[j, c])
            cp.start()
            trio.append(cp)
        cps.append(trio)
    greet(n)
    xcp.wait()
    aq = jnp.zeros((nb, dq), f32)
    ak = jnp.zeros((nb, dh), f32)
    av = jnp.zeros((nb, dh), f32)
    for c in range(wch):
        for cp in cps[c]:
            cp.wait()
        for i in range(c * total // wch, (c + 1) * total // wch):
            read_k(i).start()
        xc = xb[:, c * rows:(c + 1) * rows]
        r = pl.ds(c * rows, rows)
        aq += jnp.dot(xc, wqb[r, :], preferred_element_type=f32)
        ak += jnp.dot(xc, wkb[r, :], preferred_element_type=f32)
        av += jnp.dot(xc, wvb[r, :], preferred_element_type=f32)
    for b in range(nb):
        pieces = [aq[b:b + 1, i * dh:(i + 1) * dh] for i in range(g)] + [ak[b:b + 1], av[b:b + 1]]
        pieces.append(jnp.zeros((8 - g - 2, dh), f32))
        tile = jnp.concatenate(pieces, axis=0).astype(bf16)
        send[b] = tile
        gat[me, b] = tile
    for i in range(early):
        read_v(i).start()
    awaited(n)
    out = []
    for d in range(1, n):
        cp = pltpu.make_async_remote_copy(
            src_ref=send, dst_ref=gat.at[me], send_sem=ssem.at[d], recv_sem=rsem.at[d],
            device_id={'sp': lax.rem(me + d, n)}, device_id_type=MESH)
        cp.start()
        out.append(cp)
    for cp in out:
        cp.wait()

    for cp in icps:
        cp.wait()
    gat_out[...] = gat[...]
    gf = gat[...].astype(f32)
    sub = lax.broadcasted_iota(jnp.int32, (nkv, 128), 0)
    lane = lax.broadcasted_iota(jnp.int32, (nkv, 128), 1)
    own = sub == (lane % heads) // g
    wrow = wide * nkv // slabs
    wch_n = npos // wide
    per = wide // ch
    first = jnp.where(own, lane // heads * (wide // slabs), 1 << 29)
    for b in range(nb):
        q = jnp.concatenate([gf[i, b, 0:g] for i in range(nkv)], axis=0)
        kn = jnp.concatenate([gf[i, b, g:g + 1] for i in range(nkv)], axis=0)
        zero = jnp.zeros_like(q)
        for s in range(slabs):
            a = jnp.concatenate([q if i == s else zero for i in range(slabs)], axis=0)
            qbd[b, s * dh:(s + 1) * dh, :] = a.T.astype(bf16)
        k16 = jnp.concatenate([kn, jnp.zeros_like(kn)], axis=0).astype(bf16)
        t = jnp.dot(k16, qbd[b, 0:dh, :], preferred_element_type=f32)[0:nkv]
        here = jnp.logical_and(pos[b] >= start, pos[b] < jnp.minimum(start + npos, lens[b]))
        limit = jnp.where(here, heads, 0)
        t = jnp.where(jnp.logical_and(own, lane < limit), t, ninf)
        snew[b] = t
        mrun[b] = t

    def scores(i, _):
        b, c = i // wch_n, i % wch_n
        for t in range(per):
            read_k(i * per + t).wait()

        @pl.when(i * per + early < total)
        def _():
            for t in range(per):
                read_v(i * per + t + early).start()

        lim = jnp.minimum(pos[b], lens[b]) - start - c * wide
        acc = None
        for s in range(0, slabs, 2):
            k2 = jnp.concatenate(
                [kbuf[b, pl.ds(pl.multiple_of((c * slabs + s + t) * wrow, wrow), wrow), :] for t in range(2)], axis=1)
            t = jnp.dot(k2, qbd[b, s * dh:(s + 2) * dh, :], preferred_element_type=f32)
            acc = t if acc is None else acc + t
        acc = acc.reshape(wrow // nkv, nkv, 128)
        left = lim - lax.broadcasted_iota(jnp.int32, acc.shape, 0)
        t = jnp.where(first[None] < left, acc, ninf)
        sc[b, pl.ds(pl.multiple_of(c * wrow, wrow), wrow), :] = t.reshape(wrow, 128)
        mrun[b] = jnp.maximum(mrun[b], t.max(0))
        return 0

    lax.fori_loop(0, nb * wch_n, scores, 0)

    def landed(i, _):
        read_v(i).wait()
        return 0

    lax.fori_loop(0, total, landed, 0)


def attend(ch, wide, slabs, pos_hbm, lens_hbm, gat, kbuf, vbuf, sc, mrun, snew, part, ko, vo, pos, lens, mall, lrun, orun, knew, vnew,
           isem, ksem, vsem, nsem):
    me = lax.axis_index('sp')
    nkv, nb, _, dh = gat.shape
    npos = kbuf.shape[1] // nkv
    nch = npos // ch
    total = nb * nch
    crow = ch * nkv
    srow = crow // slabs
    heads = 128 // slabs
    g = heads // nkv
    start = me * npos
    scale = dh ** -0.5 * LOG2E
    ninf = -jnp.inf

    icps = [pltpu.make_async_copy(pos_hbm, pos, isem.at[0]), pltpu.make_async_copy(lens_hbm, lens, isem.at[1])]
    for cp in icps:
        cp.start()

    def writes(i):
        b, r = i // nch, pl.ds(pl.multiple_of(i % nch * crow, crow), crow)
        return (pltpu.make_async_copy(kbuf.at[b, r], ko.at[b, r], ksem.at[i]),
                pltpu.make_async_copy(vbuf.at[b, r], vo.at[b, r], vsem.at[i]))

    def begin(i, _):
        for cp in writes(i):
            cp.start()
        return 0

    lax.fori_loop(0, total, begin, 0)

    gf = gat[...].astype(f32)
    lrun[...] = jnp.zeros_like(lrun)
    orun[...] = jnp.zeros_like(orun)
    for b in range(nb):
        knew[b] = jnp.concatenate([gf[i, b, g:g + 1] for i in range(nkv)], axis=0).astype(bf16)
        vnew[b] = jnp.concatenate([gf[i, b, g + 1:g + 2] for i in range(nkv)], axis=0).astype(bf16)
        m = jnp.broadcast_to(mrun[b].max(0, keepdims=True), (nkv, 128))
        k = heads
        while k < 128:
            m = jnp.maximum(m, pltpu.roll(m, k, 1))
            k *= 2
        mall[b] = m

    wrow = wide * nkv // slabs
    wch_n = npos // wide

    def mix(i, _):
        b, c = i // wch_n, i % wch_n
        lim = jnp.minimum(pos[b], lens[b]) - start - c * wide

        @pl.when(lim > 0)
        def _():
            m = mall[b]
            m = jnp.where(m == ninf, 0.0, m)
            t = sc[b, pl.ds(pl.multiple_of(c * wrow, wrow), wrow), :].reshape(wrow // nkv, nkv, 128)
            e = jnp.exp2((t - m[None]) * scale)
            lrun[b] += e.sum(0)
            et = e.reshape(wrow, 128).astype(bf16).T
            o = orun[b]
            for s in range(slabs):
                v = vbuf[b, pl.ds(pl.multiple_of((c * slabs + s) * wrow, wrow), wrow), :]
                o += jnp.dot(et[s * heads:(s + 1) * heads], v, preferred_element_type=f32)
            orun[b] = o

        return 0

    for cp in icps:
        cp.wait()
    lax.fori_loop(0, nb * wch_n, mix, 0)

    half = lax.broadcasted_iota(jnp.int32, (heads, 128), 1) < 64
    for b in range(nb):
        m = mall[b]
        e = jnp.exp2((snew[b] - jnp.where(m == ninf, 0.0, m)) * scale)
        pad = jnp.zeros_like(e)
        e16 = jnp.concatenate([e, pad], axis=0).astype(bf16)
        v16 = jnp.concatenate([vnew[b].astype(f32), pad], axis=0).astype(bf16)
        o = orun[b] + lax.dot_general(e16, v16, (((0,), (0,)), ((), ())), preferred_element_type=f32)[0:heads]
        l = jnp.broadcast_to((lrun[b] + e).sum(0, keepdims=True), (nkv, 128))
        k = heads
        while k < 128:
            l = l + pltpu.roll(l, k, 1)
            k *= 2
        lt = jnp.broadcast_to(l[0:1], (128, 128)).T[0:heads]
        mt = jnp.broadcast_to(m[0:1] * scale, (128, 128)).T[0:heads]
        ml = jnp.where(half, mt, lt)
        for i in range(nkv):
            part[i, 0, b * g:(b + 1) * g, :] = o[i * g:(i + 1) * g, :]
            part[i, 1, b * g:(b + 1) * g, :] = ml[i * g:(i + 1) * g, :]

    def rows(b):
        r = pl.ds(pl.multiple_of((pos[b] - start) * nkv, nkv), nkv)
        return (pltpu.make_async_copy(knew.at[b], ko.at[b, r], nsem.at[b, 0]),
                pltpu.make_async_copy(vnew.at[b], vo.at[b, r], nsem.at[b, 1]))

    def written(i, _):
        for cp in writes(i):
            cp.wait()
        b = i // nch
        p = pos[b] - start - i % nch * ch

        @pl.when(jnp.logical_and(p >= 0, p < ch))
        def _():
            for cp in rows(b):
                cp.start()

        return 0

    lax.fori_loop(0, total, written, 0)
    for b in range(nb):
        p = pos[b] - start

        @pl.when(jnp.logical_and(p >= 0, p < npos))
        def _():
            for cp in rows(b):
                cp.wait()


def combine(n, nb, ych, part, wo, y, wob, rbuf, xs, ybuf, wsem, ssem, rsem, ysem, zsem):
    me = lax.axis_index('sp')
    cols = wo.shape[1] // ych
    cps = []
    for c in range(ych):
        cp = pltpu.make_async_copy(wo.at[:, pl.ds(c * cols, cols)], wob.at[c], wsem.at[c])
        cp.start()
        cps.append(cp)
    greet(n)
    awaited(n)
    out = []
    for d in range(1, n):
        peer = lax.rem(me + d, n)
        cp = pltpu.make_async_remote_copy(
            src_ref=part.at[peer], dst_ref=rbuf.at[me], send_sem=ssem.at[d], recv_sem=rsem.at[d],
            device_id={'sp': peer}, device_id_type=MESH)
        cp.start()
        out.append(cp)
    rbuf[me] = part[me]
    for cp in out:
        cp.wait()
    o = rbuf[:, 0]
    ml = rbuf[:, 1]
    m = jnp.broadcast_to(ml[:, :, 0:1], o.shape)
    l = jnp.broadcast_to(ml[:, :, 64:65], o.shape)
    a = jnp.exp2(m - m.max(0)[None])
    out8 = (a * o).sum(0) / (a * l).sum(0)
    g = out8.shape[0] // nb
    dh = out8.shape[1]
    xs[...] = jnp.zeros_like(xs)
    for b in range(nb):
        for j in range(g):
            xs[b:b + 1, j * dh:(j + 1) * dh] = out8[b * g + j:b * g + j + 1]
    xl = xs[...].astype(bf16)
    sent = []
    for c in range(ych):
        cps[c].wait()
        ybuf[me, c] = jnp.dot(xl, wob[c], preferred_element_type=f32)[0:nb]
        for d in range(1, n):
            cp = pltpu.make_async_remote_copy(
                src_ref=ybuf.at[me, c], dst_ref=ybuf.at[me, c], send_sem=ysem.at[c, d], recv_sem=zsem.at[c, d],
                device_id={'sp': lax.rem(me + d, n)}, device_id_type=MESH)
            cp.start()
            sent.append(cp)
    for cp in sent:
        cp.wait()
    for c in range(ych):
        t = ybuf[0, c]
        for i in range(1, n):
            t = t + ybuf[i, c]
        y[:, c * cols:(c + 1) * cols] = t.astype(bf16)


def solution(mesh):
    n = mesh.shape['sp']

    def local(x, wq, wk, wv, wo, kc, vc, pos, lens):
        nb, npos, nkv, dh = kc.shape
        dm = x.shape[1]
        dq = wq.shape[1] // n
        dma = pltpu.SemaphoreType.DMA
        kc = kc.reshape(nb, npos * nkv, dh)
        vc = vc.reshape(nb, npos * nkv, dh)
        wch, ch, wide, slabs, early = 8, 512, 1024, 4, 8
        nch = npos // ch
        small = jax.ShapeDtypeStruct((nb, nkv, 128), f32)
        gat, kbuf, vbuf, sc, mrun, snew = pl.pallas_call(
            functools.partial(lookup, n, wch, ch, wide, slabs, early),
            name='lookup',
            out_shape=(jax.ShapeDtypeStruct((n, nb, 8, dh), bf16), pltpu.VMEM(kc.shape, bf16), pltpu.VMEM(vc.shape, bf16),
                       pltpu.VMEM((nb, npos * nkv // slabs, 128), f32), small, small),
            in_specs=[ANY] * 8,
            out_specs=(VMEM,) * 6,
            scratch_shapes=[
                pltpu.SMEM((nb,), jnp.int32), pltpu.SMEM((nb,), jnp.int32),
                pltpu.VMEM(x.shape, bf16), pltpu.VMEM((dm, dq), bf16), pltpu.VMEM((dm, dh), bf16), pltpu.VMEM((dm, dh), bf16),
                pltpu.VMEM((nb, 8, dh), bf16), pltpu.VMEM((n, nb, 8, dh), bf16), pltpu.VMEM((nb, slabs * dh, 128), bf16),
                dma((2,)), dma, dma((3, wch)), dma((nb * nch,)), dma((nb * nch,)), dma((n,)), dma((n,))],
            compiler_params=pltpu.CompilerParams(collective_id=0, has_side_effects=True, vmem_limit_bytes=12 * MIB),
        )(*(pltpu.with_memory_space_constraint(t, pltpu.HBM) for t in (pos, lens, x, wq, wk, wv, kc, vc)))

        part, ko, vo = pl.pallas_call(
            functools.partial(attend, ch, wide, slabs),
            name='attend',
            out_shape=(jax.ShapeDtypeStruct((n, 2, 8, dh), f32), pltpu.HBM(kc.shape, bf16), pltpu.HBM(vc.shape, bf16)),
            in_specs=[ANY] * 2 + [VMEM] * 6,
            out_specs=(VMEM, ANY, ANY),
            scratch_shapes=[
                pltpu.SMEM((nb,), jnp.int32), pltpu.SMEM((nb,), jnp.int32),
                pltpu.VMEM((nb, nkv, 128), f32), pltpu.VMEM((nb, nkv, 128), f32), pltpu.VMEM((nb, 128 // slabs, dh), f32),
                pltpu.VMEM((nb, nkv, dh), bf16), pltpu.VMEM((nb, nkv, dh), bf16),
                dma((2,)), dma((nb * nch,)), dma((nb * nch,)), dma((nb, 2))],
            compiler_params=pltpu.CompilerParams(vmem_limit_bytes=12 * MIB),
        )(*(pltpu.with_memory_space_constraint(t, pltpu.HBM) for t in (pos, lens)), gat, kbuf, vbuf, sc, mrun, snew)

        ych = 4
        cols = wo.shape[1] // ych
        y = pl.pallas_call(
            functools.partial(combine, n, nb, ych),
            name='combine',
            out_shape=jax.ShapeDtypeStruct((nb, wo.shape[1]), bf16),
            in_specs=[VMEM, ANY],
            out_specs=VMEM,
            scratch_shapes=[
                pltpu.VMEM((ych, wo.shape[0], cols), bf16), pltpu.VMEM((n, 2, 8, dh), f32), pltpu.VMEM((8, wo.shape[0]), f32),
                pltpu.VMEM((n, ych, nb, cols), f32),
                dma((ych,)), dma((n,)), dma((n,)), dma((ych, n)), dma((ych, n))],
            compiler_params=pltpu.CompilerParams(collective_id=1, has_side_effects=True, vmem_limit_bytes=8 * MIB),
        )(part, pltpu.with_memory_space_constraint(wo, pltpu.HBM))
        shape = (nb, npos, nkv, dh)
        return y, ko.reshape(shape), vo.reshape(shape)

    cache = P('dp', 'sp', None, None)
    return jax.shard_map(
        local, mesh=mesh,
        in_specs=(P('dp', None), P(None, None), P(None, None), P(None, None), P('sp', None),
                  cache, cache, P('dp'), P('dp')),
        out_specs=(P('dp', None), cache, cache),
        check_vma=False)
```

```python
import functools

import jax
import jax.numpy as jnp
from jax import lax
from jax.experimental import pallas as pl
from jax.experimental.pallas import tpu as pltpu
from jax.sharding import PartitionSpec as P

MESH = pl.DeviceIdType.MESH
ANY = pl.BlockSpec(memory_space=pl.ANY)
VMEM = pl.BlockSpec(memory_space=pltpu.VMEM)
SMEM = pl.BlockSpec(memory_space=pltpu.SMEM)
f32 = jnp.float32
bf16 = jnp.bfloat16
LOG2E = 1.4426950408889634
MIB = 1 << 20


def greet(n):
    me = lax.axis_index('sp')
    barrier = pltpu.get_barrier_semaphore()
    for d in range(1, n):
        pl.semaphore_signal(barrier, inc=1, device_id={'sp': lax.rem(me + d, n)}, device_id_type=MESH)


def awaited(n):
    pl.semaphore_wait(pltpu.get_barrier_semaphore(), n - 1)


def lookup(n, wch, ch, wide, slabs, early, pos_hbm, lens_hbm, x, wq, wk, wv, kc, vc, gat_out, kbuf, vbuf, sc, mrun, snew,
           pos, lens, xb, wqb, wkb, wvb, send, gat, qbd, isem, xsem, wsem, ksem, vsem, ssem, rsem):
    me = lax.axis_index('sp')
    nb, dm = xb.shape
    dq, dh = wqb.shape[1], wkb.shape[1]
    rows = dm // wch
    g = dq // dh
    nkv = n
    npos = kbuf.shape[1] // nkv
    nch = npos // ch
    total = nb * nch
    crow = ch * nkv
    srow = crow // slabs
    heads = 128 // slabs
    start = me * npos
    ninf = -jnp.inf

    def chunk(i):
        return i // nch, pl.ds(pl.multiple_of(i % nch * crow, crow), crow)

    def read_k(i):
        b, r = chunk(i)
        return pltpu.make_async_copy(kc.at[b, r], kbuf.at[b, r], ksem.at[i])

    def read_v(i):
        b, r = chunk(i)
        return pltpu.make_async_copy(vc.at[b, r], vbuf.at[b, r], vsem.at[i])

    xcp = pltpu.make_async_copy(x, xb, xsem)
    xcp.start()
    icps = [pltpu.make_async_copy(pos_hbm, pos, isem.at[0]), pltpu.make_async_copy(lens_hbm, lens, isem.at[1])]
    for cp in icps:
        cp.start()
    cps = []
    for c in range(wch):
        r = pl.ds(c * rows, rows)
        trio = []
        for j, (w, buf, cols) in enumerate(((wq, wqb, dq), (wk, wkb, dh), (wv, wvb, dh))):
            cp = pltpu.make_async_copy(w.at[r, pl.ds(pl.multiple_of(me * cols, 128), cols)], buf.at[r], wsem.at[j, c])
            cp.start()
            trio.append(cp)
        cps.append(trio)
    greet(n)
    xcp.wait()
    aq = jnp.zeros((nb, dq), f32)
    ak = jnp.zeros((nb, dh), f32)
    av = jnp.zeros((nb, dh), f32)
    for c in range(wch):
        for cp in cps[c]:
            cp.wait()
        for i in range(c * total // wch, (c + 1) * total // wch):
            read_k(i).start()
        xc = xb[:, c * rows:(c + 1) * rows]
        r = pl.ds(c * rows, rows)
        aq += jnp.dot(xc, wqb[r, :], preferred_element_type=f32)
        ak += jnp.dot(xc, wkb[r, :], preferred_element_type=f32)
        av += jnp.dot(xc, wvb[r, :], preferred_element_type=f32)
    for b in range(nb):
        pieces = [aq[b:b + 1, i * dh:(i + 1) * dh] for i in range(g)] + [ak[b:b + 1], av[b:b + 1]]
        pieces.append(jnp.zeros((8 - g - 2, dh), f32))
        tile = jnp.concatenate(pieces, axis=0).astype(bf16)
        send[b] = tile
        gat[me, b] = tile
    for i in range(early):
        read_v(i).start()
    awaited(n)
    out = []
    for d in range(1, n):
        cp = pltpu.make_async_remote_copy(
            src_ref=send, dst_ref=gat.at[me], send_sem=ssem.at[d], recv_sem=rsem.at[d],
            device_id={'sp': lax.rem(me + d, n)}, device_id_type=MESH)
        cp.start()
        out.append(cp)
    for cp in out:
        cp.wait()

    for cp in icps:
        cp.wait()
    gat_out[...] = gat[...]
    gf = gat[...].astype(f32)
    sub = lax.broadcasted_iota(jnp.int32, (nkv, 128), 0)
    lane = lax.broadcasted_iota(jnp.int32, (nkv, 128), 1)
    own = sub == (lane % heads) // g
    wrow = wide * nkv // slabs
    wch_n = npos // wide
    per = wide // ch
    first = jnp.where(own, lane // heads * (wide // slabs), 1 << 29)
    for b in range(nb):
        q = jnp.concatenate([gf[i, b, 0:g] for i in range(nkv)], axis=0)
        kn = jnp.concatenate([gf[i, b, g:g + 1] for i in range(nkv)], axis=0)
        zero = jnp.zeros_like(q)
        for s in range(slabs):
            a = jnp.concatenate([q if i == s else zero for i in range(slabs)], axis=0)
            qbd[b, s * dh:(s + 1) * dh, :] = a.T.astype(bf16)
        k16 = jnp.concatenate([kn, jnp.zeros_like(kn)], axis=0).astype(bf16)
        t = jnp.dot(k16, qbd[b, 0:dh, :], preferred_element_type=f32)[0:nkv]
        here = jnp.logical_and(pos[b] >= start, pos[b] < jnp.minimum(start + npos, lens[b]))
        limit = jnp.where(here, heads, 0)
        t = jnp.where(jnp.logical_and(own, lane < limit), t, ninf)
        snew[b] = t
        mrun[b] = t

    def scores(i, _):
        b, c = i // wch_n, i % wch_n
        for t in range(per):
            read_k(i * per + t).wait()

        @pl.when(i * per + early < total)
        def _():
            for t in range(per):
                read_v(i * per + t + early).start()

        lim = jnp.minimum(pos[b], lens[b]) - start - c * wide
        acc = None
        for s in range(0, slabs, 2):
            k2 = jnp.concatenate(
                [kbuf[b, pl.ds(pl.multiple_of((c * slabs + s + t) * wrow, wrow), wrow), :] for t in range(2)], axis=1)
            t = jnp.dot(k2, qbd[b, s * dh:(s + 2) * dh, :], preferred_element_type=f32)
            acc = t if acc is None else acc + t
        acc = acc.reshape(wrow // nkv, nkv, 128)
        left = lim - lax.broadcasted_iota(jnp.int32, acc.shape, 0)
        t = jnp.where(first[None] < left, acc, ninf)
        sc[b, pl.ds(pl.multiple_of(c * wrow, wrow), wrow), :] = t.reshape(wrow, 128)
        mrun[b] = jnp.maximum(mrun[b], t.max(0))
        return 0

    lax.fori_loop(0, nb * wch_n, scores, 0)

    def landed(i, _):
        read_v(i).wait()
        return 0

    lax.fori_loop(0, total, landed, 0)


def attend(ch, wide, slabs, pos_hbm, lens_hbm, gat, kbuf, vbuf, sc, mrun, snew, part, ko, pos, lens, mall, lrun, orun, knew, isem, ksem, nsem):
    me = lax.axis_index('sp')
    nkv, nb, _, dh = gat.shape
    npos = kbuf.shape[1] // nkv
    nch = npos // ch
    total = nb * nch
    crow = ch * nkv
    srow = crow // slabs
    heads = 128 // slabs
    g = heads // nkv
    start = me * npos
    scale = dh ** -0.5 * LOG2E
    ninf = -jnp.inf

    icps = [pltpu.make_async_copy(pos_hbm, pos, isem.at[0]), pltpu.make_async_copy(lens_hbm, lens, isem.at[1])]
    for cp in icps:
        cp.start()

    def write_k(i):
        b, r = i // nch, pl.ds(pl.multiple_of(i % nch * crow, crow), crow)
        return pltpu.make_async_copy(kbuf.at[b, r], ko.at[b, r], ksem.at[i])

    def begin(i, _):
        write_k(i).start()
        return 0

    lax.fori_loop(0, total, begin, 0)

    gf = gat[...].astype(f32)
    lrun[...] = jnp.zeros_like(lrun)
    orun[...] = jnp.zeros_like(orun)
    for b in range(nb):
        knew[b] = jnp.concatenate([gf[i, b, g:g + 1] for i in range(nkv)], axis=0).astype(bf16)
        m = jnp.broadcast_to(mrun[b].max(0, keepdims=True), (nkv, 128))
        k = heads
        while k < 128:
            m = jnp.maximum(m, pltpu.roll(m, k, 1))
            k *= 2
        mall[b] = m

    wrow = wide * nkv // slabs
    wch_n = npos // wide

    def mix(i, _):
        b, c = i // wch_n, i % wch_n
        lim = jnp.minimum(pos[b], lens[b]) - start - c * wide

        @pl.when(lim > 0)
        def _():
            m = mall[b]
            m = jnp.where(m == ninf, 0.0, m)
            t = sc[b, pl.ds(pl.multiple_of(c * wrow, wrow), wrow), :].reshape(wrow // nkv, nkv, 128)
            e = jnp.exp2((t - m[None]) * scale)
            lrun[b] += e.sum(0)
            et = e.reshape(wrow, 128).astype(bf16).T
            o = orun[b]
            for s in range(slabs):
                v = vbuf[b, pl.ds(pl.multiple_of((c * slabs + s) * wrow, wrow), wrow), :]
                o += jnp.dot(et[s * heads:(s + 1) * heads], v, preferred_element_type=f32)
            orun[b] = o

        return 0

    for cp in icps:
        cp.wait()
    lax.fori_loop(0, nb * wch_n, mix, 0)

    half = lax.broadcasted_iota(jnp.int32, (heads, 128), 1) < 64
    for b in range(nb):
        m = mall[b]
        e = jnp.exp2((snew[b] - jnp.where(m == ninf, 0.0, m)) * scale)
        pad = jnp.zeros_like(e)
        e16 = jnp.concatenate([e, pad], axis=0).astype(bf16)
        v16 = jnp.concatenate([gf[i, b, g + 1:g + 2] for i in range(nkv)] + [pad], axis=0).astype(bf16)
        o = orun[b] + lax.dot_general(e16, v16, (((0,), (0,)), ((), ())), preferred_element_type=f32)[0:heads]
        l = jnp.broadcast_to((lrun[b] + e).sum(0, keepdims=True), (nkv, 128))
        k = heads
        while k < 128:
            l = l + pltpu.roll(l, k, 1)
            k *= 2
        lt = jnp.broadcast_to(l[0:1], (128, 128)).T[0:heads]
        mt = jnp.broadcast_to(m[0:1] * scale, (128, 128)).T[0:heads]
        ml = jnp.where(half, mt, lt)
        for i in range(nkv):
            part[i, 0, b * g:(b + 1) * g, :] = o[i * g:(i + 1) * g, :]
            part[i, 1, b * g:(b + 1) * g, :] = ml[i * g:(i + 1) * g, :]

    def row(b):
        r = pl.ds(pl.multiple_of((pos[b] - start) * nkv, nkv), nkv)
        return pltpu.make_async_copy(knew.at[b], ko.at[b, r], nsem.at[b])

    def written(i, _):
        write_k(i).wait()
        b = i // nch
        p = pos[b] - start - i % nch * ch

        @pl.when(jnp.logical_and(p >= 0, p < ch))
        def _():
            row(b).start()

        return 0

    lax.fori_loop(0, total, written, 0)
    for b in range(nb):
        p = pos[b] - start

        @pl.when(jnp.logical_and(p >= 0, p < npos))
        def _():
            row(b).wait()


def copy_v(ch, pos_hbm, gat, vbuf, after, vo, pos, vnew, isem, vsem, nsem):
    del after
    me = lax.axis_index('sp')
    nkv, nb, _, dh = gat.shape
    npos = vbuf.shape[1] // nkv
    nch = npos // ch
    total = nb * nch
    crow = ch * nkv
    g = gat.shape[2] // 2
    start = me * npos

    def write_v(i):
        b, r = i // nch, pl.ds(pl.multiple_of(i % nch * crow, crow), crow)
        return pltpu.make_async_copy(vbuf.at[b, r], vo.at[b, r], vsem.at[i])

    icp = pltpu.make_async_copy(pos_hbm, pos, isem)
    icp.start()

    def begin(i, _):
        write_v(i).start()
        return 0

    lax.fori_loop(0, total, begin, 0)
    gf = gat[...].astype(f32)
    for b in range(nb):
        vnew[b] = jnp.concatenate([gf[i, b, g + 1:g + 2] for i in range(nkv)], axis=0).astype(bf16)
    icp.wait()

    def row(b):
        r = pl.ds(pl.multiple_of((pos[b] - start) * nkv, nkv), nkv)
        return pltpu.make_async_copy(vnew.at[b], vo.at[b, r], nsem.at[b])

    def written(i, _):
        write_v(i).wait()
        b = i // nch
        p = pos[b] - start - i % nch * ch

        @pl.when(jnp.logical_and(p >= 0, p < ch))
        def _():
            row(b).start()

        return 0

    lax.fori_loop(0, total, written, 0)
    for b in range(nb):
        p = pos[b] - start

        @pl.when(jnp.logical_and(p >= 0, p < npos))
        def _():
            row(b).wait()


def combine(n, nb, ych, part, wo, ys, wob, rbuf, xs, mine, twin, wsem, ssem, rsem, ysem, zsem):
    me = lax.axis_index('sp')
    cols = wo.shape[1] // ych
    cps = []
    for c in range(ych):
        cp = pltpu.make_async_copy(wo.at[:, pl.ds(c * cols, cols)], wob.at[c], wsem.at[c])
        cp.start()
        cps.append(cp)
    greet(n)
    awaited(n)
    out = []
    for d in range(1, n):
        peer = lax.rem(me + d, n)
        cp = pltpu.make_async_remote_copy(
            src_ref=part.at[peer], dst_ref=rbuf.at[me], send_sem=ssem.at[d], recv_sem=rsem.at[d],
            device_id={'sp': peer}, device_id_type=MESH)
        cp.start()
        out.append(cp)
    rbuf[me] = part[me]
    for cp in out:
        cp.wait()
    o = rbuf[:, 0]
    ml = rbuf[:, 1]
    m = jnp.broadcast_to(ml[:, :, 0:1], o.shape)
    l = jnp.broadcast_to(ml[:, :, 64:65], o.shape)
    a = jnp.exp2(m - m.max(0)[None])
    out8 = (a * o).sum(0) / (a * l).sum(0)
    g = out8.shape[0] // nb
    dh = out8.shape[1]
    xs[...] = jnp.zeros_like(xs)
    for b in range(nb):
        for j in range(g):
            xs[b:b + 1, j * dh:(j + 1) * dh] = out8[b * g + j:b * g + j + 1]
    xl = xs[...].astype(bf16)
    sent = []
    for c in range(ych):
        cps[c].wait()
        mine[c] = jnp.dot(xl, wob[c], preferred_element_type=f32)[0:nb]
        cp = pltpu.make_async_remote_copy(
            src_ref=mine.at[c], dst_ref=twin.at[c], send_sem=ysem.at[c], recv_sem=zsem.at[c],
            device_id={'sp': me + 1 - 2 * lax.rem(me, 2)}, device_id_type=MESH)
        cp.start()
        sent.append(cp)
    for c in range(ych):
        sent[c].wait()
        ys[:, c * cols:(c + 1) * cols] = mine[c] + twin[c]


def add4(a, b, c, d, y):
    y[...] = ((a[...] + b[...]) + (c[...] + d[...])).astype(bf16)


def solution(mesh):
    n = mesh.shape['sp']

    def local(x, wq, wk, wv, wo, kc, vc, pos, lens):
        nb, npos, nkv, dh = kc.shape
        dm = x.shape[1]
        dq = wq.shape[1] // n
        dma = pltpu.SemaphoreType.DMA
        kc = kc.reshape(nb, npos * nkv, dh)
        vc = vc.reshape(nb, npos * nkv, dh)
        wch, ch, wide, slabs, early = 8, 512, 1024, 4, 8
        nch = npos // ch
        small = jax.ShapeDtypeStruct((nb, nkv, 128), f32)
        gat, kbuf, vbuf, sc, mrun, snew = pl.pallas_call(
            functools.partial(lookup, n, wch, ch, wide, slabs, early),
            name='lookup',
            out_shape=(jax.ShapeDtypeStruct((n, nb, 8, dh), bf16), pltpu.VMEM(kc.shape, bf16), pltpu.VMEM(vc.shape, bf16),
                       pltpu.VMEM((nb, npos * nkv // slabs, 128), f32), small, small),
            in_specs=[ANY] * 8,
            out_specs=(VMEM,) * 6,
            scratch_shapes=[
                pltpu.SMEM((nb,), jnp.int32), pltpu.SMEM((nb,), jnp.int32),
                pltpu.VMEM(x.shape, bf16), pltpu.VMEM((dm, dq), bf16), pltpu.VMEM((dm, dh), bf16), pltpu.VMEM((dm, dh), bf16),
                pltpu.VMEM((nb, 8, dh), bf16), pltpu.VMEM((n, nb, 8, dh), bf16), pltpu.VMEM((nb, slabs * dh, 128), bf16),
                dma((2,)), dma, dma((3, wch)), dma((nb * nch,)), dma((nb * nch,)), dma((n,)), dma((n,))],
            compiler_params=pltpu.CompilerParams(collective_id=0, has_side_effects=True, vmem_limit_bytes=12 * MIB),
        )(*(pltpu.with_memory_space_constraint(t, pltpu.HBM) for t in (pos, lens, x, wq, wk, wv, kc, vc)))

        part, ko = pl.pallas_call(
            functools.partial(attend, ch, wide, slabs),
            name='attend',
            out_shape=(jax.ShapeDtypeStruct((n, 2, 8, dh), f32), pltpu.HBM(kc.shape, bf16)),
            in_specs=[ANY] * 2 + [VMEM] * 6,
            out_specs=(VMEM, ANY),
            scratch_shapes=[
                pltpu.SMEM((nb,), jnp.int32), pltpu.SMEM((nb,), jnp.int32),
                pltpu.VMEM((nb, nkv, 128), f32), pltpu.VMEM((nb, nkv, 128), f32), pltpu.VMEM((nb, 128 // slabs, dh), f32),
                pltpu.VMEM((nb, nkv, dh), bf16), dma((2,)), dma((nb * nch,)), dma((nb,))],
            compiler_params=pltpu.CompilerParams(vmem_limit_bytes=12 * MIB),
        )(*(pltpu.with_memory_space_constraint(t, pltpu.HBM) for t in (pos, lens)), gat, kbuf, vbuf, sc, mrun, snew)

        ych = 4
        cols = wo.shape[1] // ych
        ys = pl.pallas_call(
            functools.partial(combine, n, nb, ych),
            name='combine',
            out_shape=jax.ShapeDtypeStruct((nb, wo.shape[1]), f32),
            in_specs=[VMEM, ANY],
            out_specs=VMEM,
            scratch_shapes=[
                pltpu.VMEM((ych, wo.shape[0], cols), bf16), pltpu.VMEM((n, 2, 8, dh), f32), pltpu.VMEM((8, wo.shape[0]), f32),
                pltpu.VMEM((ych, nb, cols), f32), pltpu.VMEM((ych, nb, cols), f32),
                dma((ych,)), dma((n,)), dma((n,)), dma((ych,)), dma((ych,))],
            compiler_params=pltpu.CompilerParams(collective_id=1, has_side_effects=True, vmem_limit_bytes=12 * MIB),
        )(part, pltpu.with_memory_space_constraint(wo, pltpu.HBM))
        others = [lax.ppermute(ys, 'sp', [(i, i ^ d) for i in range(n)]) for d in (2, 4, 6)]
        vo = pl.pallas_call(
            functools.partial(copy_v, ch),
            name='copy_v',
            out_shape=pltpu.HBM(vc.shape, bf16),
            in_specs=[ANY] + [VMEM] * 3,
            out_specs=ANY,
            scratch_shapes=[
                pltpu.SMEM((nb,), jnp.int32), pltpu.VMEM((nb, nkv, dh), bf16), dma, dma((nb * nch,)), dma((nb,))],
            compiler_params=pltpu.CompilerParams(vmem_limit_bytes=1 * MIB),
            cost_estimate=pl.CostEstimate(flops=10 ** 10, bytes_accessed=24 * MIB, transcendentals=0),
        )(pltpu.with_memory_space_constraint(pos, pltpu.HBM), gat, vbuf, ys)
        y = pl.pallas_call(
            add4,
            name='add4',
            out_shape=jax.ShapeDtypeStruct((nb, wo.shape[1]), bf16),
            in_specs=[VMEM] * 4,
            out_specs=VMEM,
            compiler_params=pltpu.CompilerParams(vmem_limit_bytes=2 * MIB),
        )(ys, *others)
        shape = (nb, npos, nkv, dh)
        return y, ko.reshape(shape), vo.reshape(shape)

    cache = P('dp', 'sp', None, None)
    return jax.shard_map(
        local, mesh=mesh,
        in_specs=(P('dp', None), P(None, None), P(None, None), P(None, None), P('sp', None),
                  cache, cache, P('dp'), P('dp')),
        out_specs=(P('dp', None), cache, cache),
        check_vma=False)
```

```python
import functools

import jax
import jax.numpy as jnp
from jax import lax
from jax.experimental import pallas as pl
from jax.experimental.pallas import tpu as pltpu
from jax.sharding import PartitionSpec as P

MESH = pl.DeviceIdType.MESH
ANY = pl.BlockSpec(memory_space=pl.ANY)
VMEM = pl.BlockSpec(memory_space=pltpu.VMEM)
SMEM = pl.BlockSpec(memory_space=pltpu.SMEM)
f32 = jnp.float32
bf16 = jnp.bfloat16
LOG2E = 1.4426950408889634
MIB = 1 << 20


def greet(n):
    me = lax.axis_index('sp')
    barrier = pltpu.get_barrier_semaphore()
    for d in range(1, n):
        pl.semaphore_signal(barrier, inc=1, device_id={'sp': lax.rem(me + d, n)}, device_id_type=MESH)


def awaited(n):
    pl.semaphore_wait(pltpu.get_barrier_semaphore(), n - 1)


def lookup(n, wch, ch, wide, slabs, early, kpre, pos_hbm, lens_hbm, x, wq, wk, wv, kc, vc, gat_out, kbuf, vbuf, sc, mrun, snew,
           pos, lens, xb, wqb, wab, send, gat, qbd, isem, xsem, wsem, ksem, vsem, ssem, rsem):
    me = lax.axis_index('sp')
    nb, dm = xb.shape
    dq, dh, da = wqb.shape[1], gat.shape[3], wab.shape[1]
    rows = dm // wch
    g = dq // dh
    nkv = n
    npos = kbuf.shape[1] // nkv
    nch = npos // ch
    total = nb * nch
    crow = ch * nkv
    srow = crow // slabs
    heads = 128 // slabs
    start = me * npos
    ninf = -jnp.inf

    def chunk(i):
        return i // nch, pl.ds(pl.multiple_of(i % nch * crow, crow), crow)

    def read_k(i):
        b, r = chunk(i)
        return pltpu.make_async_copy(kc.at[b, r], kbuf.at[b, r], ksem.at[i])

    def read_v(i):
        b, r = chunk(i)
        return pltpu.make_async_copy(vc.at[b, r], vbuf.at[b, r], vsem.at[i])

    xcp = pltpu.make_async_copy(x, xb, xsem)
    xcp.start()
    icps = [pltpu.make_async_copy(pos_hbm, pos, isem.at[0]), pltpu.make_async_copy(lens_hbm, lens, isem.at[1])]
    for cp in icps:
        cp.start()
    even = lax.rem(me, 2) == 0

    def read_q(c):
        r = pl.ds(c * rows, rows)
        return pltpu.make_async_copy(wq.at[r, pl.ds(pl.multiple_of(me * dq, 128), dq)], wqb.at[r], wsem.at[0, c])

    def read_a(w, c):
        r = pl.ds(c * rows, rows)
        return pltpu.make_async_copy(w.at[r, pl.ds(pl.multiple_of(me // 2 * da, 128), da)], wab.at[r], wsem.at[1, c])

    for c in range(wch):
        read_q(c).start()

    @pl.when(even)
    def _():
        for c in range(wch):
            read_a(wk, c).start()

    @pl.when(jnp.logical_not(even))
    def _():
        for c in range(wch):
            read_a(wv, c).start()

    for i in range(kpre):
        read_k(i).start()
    greet(n)
    xcp.wait()
    aq = jnp.zeros((nb, dq), f32)
    aa = jnp.zeros((nb, da), f32)
    for c in range(wch):
        read_q(c).wait()
        read_a(wk, c).wait()
        for i in range(kpre + c * (total - kpre) // wch, kpre + (c + 1) * (total - kpre) // wch):
            read_k(i).start()
        xc = xb[:, c * rows:(c + 1) * rows]
        r = pl.ds(c * rows, rows)
        aq += jnp.dot(xc, wqb[r, :], preferred_element_type=f32)
        aa += jnp.dot(xc, wab[r, :], preferred_element_type=f32)
    for b in range(nb):
        pieces = [aq[b:b + 1, i * dh:(i + 1) * dh] for i in range(g)] + [aa[b:b + 1, i * dh:(i + 1) * dh] for i in range(2)]
        pieces.append(jnp.zeros((8 - g - 2, dh), f32))
        tile = jnp.concatenate(pieces, axis=0).astype(bf16)
        send[b] = tile
        gat[me, b] = tile
    for i in range(early):
        read_v(i).start()
    awaited(n)
    out = []
    for d in range(1, n):
        cp = pltpu.make_async_remote_copy(
            src_ref=send, dst_ref=gat.at[me], send_sem=ssem.at[d], recv_sem=rsem.at[d],
            device_id={'sp': lax.rem(me + d, n)}, device_id_type=MESH)
        cp.start()
        out.append(cp)
    for cp in out:
        cp.wait()

    for cp in icps:
        cp.wait()
    gat_out[...] = gat[...]
    gf = gat[...].astype(f32)
    sub = lax.broadcasted_iota(jnp.int32, (nkv, 128), 0)
    lane = lax.broadcasted_iota(jnp.int32, (nkv, 128), 1)
    own = sub == (lane % heads) // g
    wrow = wide * nkv // slabs
    wch_n = npos // wide
    per = wide // ch
    first = jnp.where(own, lane // heads * (wide // slabs), 1 << 29)
    for b in range(nb):
        q = jnp.concatenate([gf[i, b, 0:g] for i in range(nkv)], axis=0)
        kn = jnp.concatenate([gf[i // 2 * 2, b, g + i % 2:g + i % 2 + 1] for i in range(nkv)], axis=0)
        zero = jnp.zeros_like(q)
        for s in range(slabs):
            a = jnp.concatenate([q if i == s else zero for i in range(slabs)], axis=0)
            qbd[b, s * dh:(s + 1) * dh, :] = a.T.astype(bf16)
        k16 = jnp.concatenate([kn, jnp.zeros_like(kn)], axis=0).astype(bf16)
        t = jnp.dot(k16, qbd[b, 0:dh, :], preferred_element_type=f32)[0:nkv]
        here = jnp.logical_and(pos[b] >= start, pos[b] < jnp.minimum(start + npos, lens[b]))
        limit = jnp.where(here, heads, 0)
        t = jnp.where(jnp.logical_and(own, lane < limit), t, ninf)
        snew[b] = t
        mrun[b] = t

    def scores(i, _):
        b, c = i // wch_n, i % wch_n
        for t in range(per):
            read_k(i * per + t).wait()

        @pl.when(i * per + early < total)
        def _():
            for t in range(per):
                read_v(i * per + t + early).start()

        lim = jnp.minimum(pos[b], lens[b]) - start - c * wide
        acc = None
        for s in range(0, slabs, 2):
            k2 = jnp.concatenate(
                [kbuf[b, pl.ds(pl.multiple_of((c * slabs + s + t) * wrow, wrow), wrow), :] for t in range(2)], axis=1)
            t = jnp.dot(k2, qbd[b, s * dh:(s + 2) * dh, :], preferred_element_type=f32)
            acc = t if acc is None else acc + t
        acc = acc.reshape(wrow // nkv, nkv, 128)
        left = lim - lax.broadcasted_iota(jnp.int32, acc.shape, 0)
        t = jnp.where(first[None] < left, acc, ninf)
        sc[b, pl.ds(pl.multiple_of(c * wrow, wrow), wrow), :] = t.reshape(wrow, 128)
        mrun[b] = jnp.maximum(mrun[b], t.max(0))
        return 0

    lax.fori_loop(0, nb * wch_n, scores, 0)

    def landed(i, _):
        read_v(i).wait()
        return 0

    lax.fori_loop(0, total, landed, 0)


def attend(ch, wide, slabs, pos_hbm, lens_hbm, gat, kbuf, vbuf, sc, mrun, snew, part, ko, vo, pos, lens, mall, lrun, orun, knew, vnew,
           isem, ksem, vsem, nsem):
    me = lax.axis_index('sp')
    nkv, nb, _, dh = gat.shape
    npos = kbuf.shape[1] // nkv
    nch = npos // ch
    total = nb * nch
    crow = ch * nkv
    srow = crow // slabs
    heads = 128 // slabs
    g = heads // nkv
    start = me * npos
    scale = dh ** -0.5 * LOG2E
    ninf = -jnp.inf

    icps = [pltpu.make_async_copy(pos_hbm, pos, isem.at[0]), pltpu.make_async_copy(lens_hbm, lens, isem.at[1])]
    for cp in icps:
        cp.start()

    def writes(i):
        b, r = i // nch, pl.ds(pl.multiple_of(i % nch * crow, crow), crow)
        return (pltpu.make_async_copy(kbuf.at[b, r], ko.at[b, r], ksem.at[i]),
                pltpu.make_async_copy(vbuf.at[b, r], vo.at[b, r], vsem.at[i]))

    def begin(i, _):
        for t, cp in enumerate(writes(i)):
            cp.start(priority=t)
        return 0

    lax.fori_loop(0, total, begin, 0)

    gf = gat[...].astype(f32)
    lrun[...] = jnp.zeros_like(lrun)
    orun[...] = jnp.zeros_like(orun)
    for b in range(nb):
        knew[b] = jnp.concatenate([gf[i // 2 * 2, b, g + i % 2:g + i % 2 + 1] for i in range(nkv)], axis=0).astype(bf16)
        vnew[b] = jnp.concatenate([gf[i // 2 * 2 + 1, b, g + i % 2:g + i % 2 + 1] for i in range(nkv)], axis=0).astype(bf16)
        m = jnp.broadcast_to(mrun[b].max(0, keepdims=True), (nkv, 128))
        k = heads
        while k < 128:
            m = jnp.maximum(m, pltpu.roll(m, k, 1))
            k *= 2
        mall[b] = m

    wrow = wide * nkv // slabs
    wch_n = npos // wide

    def mix(i, _):
        b, c = i // wch_n, i % wch_n
        lim = jnp.minimum(pos[b], lens[b]) - start - c * wide

        @pl.when(lim > 0)
        def _():
            m = mall[b]
            m = jnp.where(m == ninf, 0.0, m)
            t = sc[b, pl.ds(pl.multiple_of(c * wrow, wrow), wrow), :].reshape(wrow // nkv, nkv, 128)
            e = jnp.exp2((t - m[None]) * scale)
            lrun[b] += e.sum(0)
            et = e.reshape(wrow, 128).astype(bf16).T
            o = orun[b]
            for s in range(slabs):
                v = vbuf[b, pl.ds(pl.multiple_of((c * slabs + s) * wrow, wrow), wrow), :]
                o += jnp.dot(et[s * heads:(s + 1) * heads], v, preferred_element_type=f32)
            orun[b] = o

        return 0

    for cp in icps:
        cp.wait()
    lax.fori_loop(0, nb * wch_n, mix, 0)

    half = lax.broadcasted_iota(jnp.int32, (heads, 128), 1) < 64
    for b in range(nb):
        m = mall[b]
        e = jnp.exp2((snew[b] - jnp.where(m == ninf, 0.0, m)) * scale)
        pad = jnp.zeros_like(e)
        e16 = jnp.concatenate([e, pad], axis=0).astype(bf16)
        v16 = jnp.concatenate([vnew[b].astype(f32), pad], axis=0).astype(bf16)
        o = orun[b] + lax.dot_general(e16, v16, (((0,), (0,)), ((), ())), preferred_element_type=f32)[0:heads]
        l = jnp.broadcast_to((lrun[b] + e).sum(0, keepdims=True), (nkv, 128))
        k = heads
        while k < 128:
            l = l + pltpu.roll(l, k, 1)
            k *= 2
        lt = jnp.broadcast_to(l[0:1], (128, 128)).T[0:heads]
        mt = jnp.broadcast_to(m[0:1] * scale, (128, 128)).T[0:heads]
        ml = jnp.where(half, mt, lt)
        for i in range(nkv):
            part[i, 0, b * g:(b + 1) * g, :] = o[i * g:(i + 1) * g, :]
            part[i, 1, b * g:(b + 1) * g, :] = ml[i * g:(i + 1) * g, :]

    def rows(b):
        r = pl.ds(pl.multiple_of((pos[b] - start) * nkv, nkv), nkv)
        return (pltpu.make_async_copy(knew.at[b], ko.at[b, r], nsem.at[b, 0]),
                pltpu.make_async_copy(vnew.at[b], vo.at[b, r], nsem.at[b, 1]))

    def written(i, _):
        for cp in writes(i):
            cp.wait()
        b = i // nch
        p = pos[b] - start - i % nch * ch

        @pl.when(jnp.logical_and(p >= 0, p < ch))
        def _():
            for cp in rows(b):
                cp.start()

        return 0

    lax.fori_loop(0, total, written, 0)
    for b in range(nb):
        p = pos[b] - start

        @pl.when(jnp.logical_and(p >= 0, p < npos))
        def _():
            for cp in rows(b):
                cp.wait()


def combine(n, nb, ych, part, wo, y, wob, rbuf, xs, ybuf, wsem, ssem, rsem, ysem, zsem):
    me = lax.axis_index('sp')
    cols = wo.shape[1] // ych
    cps = []
    for c in range(ych):
        cp = pltpu.make_async_copy(wo.at[:, pl.ds(c * cols, cols)], wob.at[c], wsem.at[c])
        cp.start()
        cps.append(cp)
    greet(n)
    awaited(n)
    out = []
    for d in range(1, n):
        peer = lax.rem(me + d, n)
        cp = pltpu.make_async_remote_copy(
            src_ref=part.at[peer], dst_ref=rbuf.at[me], send_sem=ssem.at[d], recv_sem=rsem.at[d],
            device_id={'sp': peer}, device_id_type=MESH)
        cp.start()
        out.append(cp)
    rbuf[me] = part[me]
    for cp in out:
        cp.wait()
    o = rbuf[:, 0]
    ml = rbuf[:, 1]
    m = jnp.broadcast_to(ml[:, :, 0:1], o.shape)
    l = jnp.broadcast_to(ml[:, :, 64:65], o.shape)
    a = jnp.exp2(m - m.max(0)[None])
    out8 = (a * o).sum(0) / (a * l).sum(0)
    g = out8.shape[0] // nb
    dh = out8.shape[1]
    xs[...] = jnp.zeros_like(xs)
    for b in range(nb):
        for j in range(g):
            xs[b:b + 1, j * dh:(j + 1) * dh] = out8[b * g + j:b * g + j + 1]
    xl = xs[...].astype(bf16)
    sent = []
    for c in range(ych):
        cps[c].wait()
        ybuf[me, c] = jnp.dot(xl, wob[c], preferred_element_type=f32)[0:nb]
        for d in range(1, n):
            cp = pltpu.make_async_remote_copy(
                src_ref=ybuf.at[me, c], dst_ref=ybuf.at[me, c], send_sem=ysem.at[c, d], recv_sem=zsem.at[c, d],
                device_id={'sp': lax.rem(me + d, n)}, device_id_type=MESH)
            cp.start()
            sent.append(cp)
    for cp in sent:
        cp.wait()
    for c in range(ych):
        t = ybuf[0, c]
        for i in range(1, n):
            t = t + ybuf[i, c]
        y[:, c * cols:(c + 1) * cols] = t.astype(bf16)


def solution(mesh):
    n = mesh.shape['sp']

    def local(x, wq, wk, wv, wo, kc, vc, pos, lens):
        nb, npos, nkv, dh = kc.shape
        dm = x.shape[1]
        dq = wq.shape[1] // n
        dma = pltpu.SemaphoreType.DMA
        kc = kc.reshape(nb, npos * nkv, dh)
        vc = vc.reshape(nb, npos * nkv, dh)
        wch, ch, wide, slabs, early, kpre = 8, 512, 1024, 4, 8, 2
        nch = npos // ch
        small = jax.ShapeDtypeStruct((nb, nkv, 128), f32)
        gat, kbuf, vbuf, sc, mrun, snew = pl.pallas_call(
            functools.partial(lookup, n, wch, ch, wide, slabs, early, kpre),
            name='lookup',
            out_shape=(jax.ShapeDtypeStruct((n, nb, 8, dh), bf16), pltpu.VMEM(kc.shape, bf16), pltpu.VMEM(vc.shape, bf16),
                       pltpu.VMEM((nb, npos * nkv // slabs, 128), f32), small, small),
            in_specs=[ANY] * 8,
            out_specs=(VMEM,) * 6,
            scratch_shapes=[
                pltpu.SMEM((nb,), jnp.int32), pltpu.SMEM((nb,), jnp.int32),
                pltpu.VMEM(x.shape, bf16), pltpu.VMEM((dm, dq), bf16), pltpu.VMEM((dm, 2 * dh), bf16),
                pltpu.VMEM((nb, 8, dh), bf16), pltpu.VMEM((n, nb, 8, dh), bf16), pltpu.VMEM((nb, slabs * dh, 128), bf16),
                dma((2,)), dma, dma((2, wch)), dma((nb * nch,)), dma((nb * nch,)), dma((n,)), dma((n,))],
            compiler_params=pltpu.CompilerParams(collective_id=0, has_side_effects=True, vmem_limit_bytes=12 * MIB),
        )(*(pltpu.with_memory_space_constraint(t, pltpu.HBM) for t in (pos, lens, x, wq, wk, wv, kc, vc)))

        part, ko, vo = pl.pallas_call(
            functools.partial(attend, ch, wide, slabs),
            name='attend',
            out_shape=(jax.ShapeDtypeStruct((n, 2, 8, dh), f32), pltpu.HBM(kc.shape, bf16), pltpu.HBM(vc.shape, bf16)),
            in_specs=[ANY] * 2 + [VMEM] * 6,
            out_specs=(VMEM, ANY, ANY),
            scratch_shapes=[
                pltpu.SMEM((nb,), jnp.int32), pltpu.SMEM((nb,), jnp.int32),
                pltpu.VMEM((nb, nkv, 128), f32), pltpu.VMEM((nb, nkv, 128), f32), pltpu.VMEM((nb, 128 // slabs, dh), f32),
                pltpu.VMEM((nb, nkv, dh), bf16), pltpu.VMEM((nb, nkv, dh), bf16),
                dma((2,)), dma((nb * nch,)), dma((nb * nch,)), dma((nb, 2))],
            compiler_params=pltpu.CompilerParams(vmem_limit_bytes=12 * MIB),
        )(*(pltpu.with_memory_space_constraint(t, pltpu.HBM) for t in (pos, lens)), gat, kbuf, vbuf, sc, mrun, snew)

        ych = 4
        cols = wo.shape[1] // ych
        y = pl.pallas_call(
            functools.partial(combine, n, nb, ych),
            name='combine',
            out_shape=jax.ShapeDtypeStruct((nb, wo.shape[1]), bf16),
            in_specs=[VMEM, ANY],
            out_specs=VMEM,
            scratch_shapes=[
                pltpu.VMEM((ych, wo.shape[0], cols), bf16), pltpu.VMEM((n, 2, 8, dh), f32), pltpu.VMEM((8, wo.shape[0]), f32),
                pltpu.VMEM((n, ych, nb, cols), f32),
                dma((ych,)), dma((n,)), dma((n,)), dma((ych, n)), dma((ych, n))],
            compiler_params=pltpu.CompilerParams(collective_id=1, has_side_effects=True, vmem_limit_bytes=8 * MIB),
        )(part, pltpu.with_memory_space_constraint(wo, pltpu.HBM))
        shape = (nb, npos, nkv, dh)
        return y, ko.reshape(shape), vo.reshape(shape)

    cache = P('dp', 'sp', None, None)
    return jax.shard_map(
        local, mesh=mesh,
        in_specs=(P('dp', None), P(None, None), P(None, None), P(None, None), P('sp', None),
                  cache, cache, P('dp'), P('dp')),
        out_specs=(P('dp', None), cache, cache),
        check_vma=False)
```

```python
import functools

import jax
import jax.numpy as jnp
from jax import lax
from jax.experimental import pallas as pl
from jax.experimental.pallas import tpu as pltpu
from jax.sharding import PartitionSpec as P

MESH = pl.DeviceIdType.MESH
ANY = pl.BlockSpec(memory_space=pl.ANY)
VMEM = pl.BlockSpec(memory_space=pltpu.VMEM)
SMEM = pl.BlockSpec(memory_space=pltpu.SMEM)
f32 = jnp.float32
bf16 = jnp.bfloat16
LOG2E = 1.4426950408889634
MIB = 1 << 20


def greet(n):
    me = lax.axis_index('sp')
    barrier = pltpu.get_barrier_semaphore()
    for d in range(1, n):
        pl.semaphore_signal(barrier, inc=1, device_id={'sp': lax.rem(me + d, n)}, device_id_type=MESH)


def awaited(n):
    pl.semaphore_wait(pltpu.get_barrier_semaphore(), n - 1)


def lookup(n, wch, ch, kpre, x, wq, wk, wv, kc, vc, gat_out, kbuf, vbuf,
           xb, wqb, wab, send, gat, xsem, wsem, ksem, vsem, ssem, rsem):
    me = lax.axis_index('sp')
    nb, dm = xb.shape
    dq, dh, da = wqb.shape[1], gat.shape[3], wab.shape[1]
    rows = dm // wch
    g = dq // dh
    nkv = n
    npos = kbuf.shape[1] // nkv
    nch = npos // ch
    total = nb * nch
    crow = ch * nkv

    def chunk(i):
        return i // nch, pl.ds(pl.multiple_of(i % nch * crow, crow), crow)

    def read_k(i):
        b, r = chunk(i)
        return pltpu.make_async_copy(kc.at[b, r], kbuf.at[b, r], ksem.at[i])

    def read_v(i):
        b, r = chunk(i)
        return pltpu.make_async_copy(vc.at[b, r], vbuf.at[b, r], vsem.at[i])

    xcp = pltpu.make_async_copy(x, xb, xsem)
    xcp.start()
    even = lax.rem(me, 2) == 0

    def read_q(c):
        r = pl.ds(c * rows, rows)
        return pltpu.make_async_copy(wq.at[r, pl.ds(pl.multiple_of(me * dq, 128), dq)], wqb.at[r], wsem.at[0, c])

    def read_a(w, c):
        r = pl.ds(c * rows, rows)
        return pltpu.make_async_copy(w.at[r, pl.ds(pl.multiple_of(me // 2 * da, 128), da)], wab.at[r], wsem.at[1, c])

    for c in range(wch):
        read_q(c).start()

    @pl.when(even)
    def _():
        for c in range(wch):
            read_a(wk, c).start()

    @pl.when(jnp.logical_not(even))
    def _():
        for c in range(wch):
            read_a(wv, c).start()

    for i in range(kpre):
        read_k(i).start()
    greet(n)
    xcp.wait()
    aq = jnp.zeros((nb, dq), f32)
    aa = jnp.zeros((nb, da), f32)
    for c in range(wch):
        read_q(c).wait()
        read_a(wk, c).wait()
        for i in range(kpre + c * (total - kpre) // wch, kpre + (c + 1) * (total - kpre) // wch):
            read_k(i).start()
        xc = xb[:, c * rows:(c + 1) * rows]
        r = pl.ds(c * rows, rows)
        aq += jnp.dot(xc, wqb[r, :], preferred_element_type=f32)
        aa += jnp.dot(xc, wab[r, :], preferred_element_type=f32)
    for b in range(nb):
        pieces = [aq[b:b + 1, i * dh:(i + 1) * dh] for i in range(g)] + [aa[b:b + 1, i * dh:(i + 1) * dh] for i in range(2)]
        pieces.append(jnp.zeros((8 - g - 2, dh), f32))
        tile = jnp.concatenate(pieces, axis=0).astype(bf16)
        send[b] = tile
        gat[me, b] = tile
    for i in range(total):
        read_v(i).start()
    awaited(n)
    out = []
    for d in range(1, n):
        cp = pltpu.make_async_remote_copy(
            src_ref=send, dst_ref=gat.at[me], send_sem=ssem.at[d], recv_sem=rsem.at[d],
            device_id={'sp': lax.rem(me + d, n)}, device_id_type=MESH)
        cp.start()
        out.append(cp)
    for cp in out:
        cp.wait()

    gat_out[...] = gat[...]

    def landed(i, _):
        read_k(i).wait()
        read_v(i).wait()
        return 0

    lax.fori_loop(0, total, landed, 0)


def attend(ch, wide, slabs, pos_hbm, lens_hbm, gat, kbuf, vbuf, part, ko, vo, pos, lens, sc, qbd, mrun, snew, mall, lrun, orun, knew, vnew,
           isem, ksem, vsem, nsem):
    me = lax.axis_index('sp')
    nkv, nb, _, dh = gat.shape
    npos = kbuf.shape[1] // nkv
    nch = npos // ch
    total = nb * nch
    crow = ch * nkv
    srow = crow // slabs
    heads = 128 // slabs
    g = heads // nkv
    start = me * npos
    scale = dh ** -0.5 * LOG2E
    ninf = -jnp.inf

    icps = [pltpu.make_async_copy(pos_hbm, pos, isem.at[0]), pltpu.make_async_copy(lens_hbm, lens, isem.at[1])]
    for cp in icps:
        cp.start()

    def writes(i):
        b, r = i // nch, pl.ds(pl.multiple_of(i % nch * crow, crow), crow)
        return (pltpu.make_async_copy(kbuf.at[b, r], ko.at[b, r], ksem.at[i]),
                pltpu.make_async_copy(vbuf.at[b, r], vo.at[b, r], vsem.at[i]))

    def begin(i, _):
        for t, cp in enumerate(writes(i)):
            cp.start(priority=t)
        return 0

    lax.fori_loop(0, total, begin, 0)

    wrow = wide * nkv // slabs
    wch_n = npos // wide
    gf = gat[...].astype(f32)
    lrun[...] = jnp.zeros_like(lrun)
    orun[...] = jnp.zeros_like(orun)
    sub = lax.broadcasted_iota(jnp.int32, (nkv, 128), 0)
    lane = lax.broadcasted_iota(jnp.int32, (nkv, 128), 1)
    own = sub == (lane % heads) // g
    first = jnp.where(own, lane // heads * (wide // slabs), 1 << 29)
    for cp in icps:
        cp.wait()
    for b in range(nb):
        q = jnp.concatenate([gf[i, b, 0:g] for i in range(nkv)], axis=0)
        kn = jnp.concatenate([gf[i // 2 * 2, b, g + i % 2:g + i % 2 + 1] for i in range(nkv)], axis=0)
        knew[b] = kn.astype(bf16)
        vnew[b] = jnp.concatenate([gf[i // 2 * 2 + 1, b, g + i % 2:g + i % 2 + 1] for i in range(nkv)], axis=0).astype(bf16)
        zero = jnp.zeros_like(q)
        for s in range(slabs):
            a = jnp.concatenate([q if i == s else zero for i in range(slabs)], axis=0)
            qbd[b, s * dh:(s + 1) * dh, :] = a.T.astype(bf16)
        k16 = jnp.concatenate([kn, jnp.zeros_like(kn)], axis=0).astype(bf16)
        t = jnp.dot(k16, qbd[b, 0:dh, :], preferred_element_type=f32)[0:nkv]
        here = jnp.logical_and(pos[b] >= start, pos[b] < jnp.minimum(start + npos, lens[b]))
        t = jnp.where(jnp.logical_and(own, lane < jnp.where(here, heads, 0)), t, ninf)
        snew[b] = t
        mrun[b] = t

    def scores(i, _):
        b, c = i // wch_n, i % wch_n
        lim = jnp.minimum(pos[b], lens[b]) - start - c * wide

        @pl.when(lim > 0)
        def _():
            acc = None
            for s in range(0, slabs, 2):
                k2 = jnp.concatenate(
                    [kbuf[b, pl.ds(pl.multiple_of((c * slabs + s + t) * wrow, wrow), wrow), :] for t in range(2)], axis=1)
                t = jnp.dot(k2, qbd[b, s * dh:(s + 2) * dh, :], preferred_element_type=f32)
                acc = t if acc is None else acc + t
            acc = acc.reshape(wrow // nkv, nkv, 128)
            left = lim - lax.broadcasted_iota(jnp.int32, acc.shape, 0)
            t = jnp.where(first[None] < left, acc, ninf)
            sc[b, pl.ds(pl.multiple_of(c * wrow, wrow), wrow), :] = t.reshape(wrow, 128)
            mrun[b] = jnp.maximum(mrun[b], t.max(0))

        return 0

    lax.fori_loop(0, nb * wch_n, scores, 0)

    for b in range(nb):
        m = jnp.broadcast_to(mrun[b].max(0, keepdims=True), (nkv, 128))
        k = heads
        while k < 128:
            m = jnp.maximum(m, pltpu.roll(m, k, 1))
            k *= 2
        mall[b] = m

    def mix(i, _):
        b, c = i // wch_n, i % wch_n
        lim = jnp.minimum(pos[b], lens[b]) - start - c * wide

        @pl.when(lim > 0)
        def _():
            m = mall[b]
            m = jnp.where(m == ninf, 0.0, m)
            t = sc[b, pl.ds(pl.multiple_of(c * wrow, wrow), wrow), :].reshape(wrow // nkv, nkv, 128)
            e = jnp.exp2((t - m[None]) * scale)
            lrun[b] += e.sum(0)
            et = e.reshape(wrow, 128).astype(bf16).T
            o = orun[b]
            for s in range(slabs):
                v = vbuf[b, pl.ds(pl.multiple_of((c * slabs + s) * wrow, wrow), wrow), :]
                o += jnp.dot(et[s * heads:(s + 1) * heads], v, preferred_element_type=f32)
            orun[b] = o

        return 0

    lax.fori_loop(0, nb * wch_n, mix, 0)

    half = lax.broadcasted_iota(jnp.int32, (heads, 128), 1) < 64
    for b in range(nb):
        m = mall[b]
        e = jnp.exp2((snew[b] - jnp.where(m == ninf, 0.0, m)) * scale)
        pad = jnp.zeros_like(e)
        e16 = jnp.concatenate([e, pad], axis=0).astype(bf16)
        v16 = jnp.concatenate([vnew[b].astype(f32), pad], axis=0).astype(bf16)
        o = orun[b] + lax.dot_general(e16, v16, (((0,), (0,)), ((), ())), preferred_element_type=f32)[0:heads]
        l = jnp.broadcast_to((lrun[b] + e).sum(0, keepdims=True), (nkv, 128))
        k = heads
        while k < 128:
            l = l + pltpu.roll(l, k, 1)
            k *= 2
        lt = jnp.broadcast_to(l[0:1], (128, 128)).T[0:heads]
        mt = jnp.broadcast_to(m[0:1] * scale, (128, 128)).T[0:heads]
        ml = jnp.where(half, mt, lt)
        for i in range(nkv):
            part[i, 0, b * g:(b + 1) * g, :] = o[i * g:(i + 1) * g, :]
            part[i, 1, b * g:(b + 1) * g, :] = ml[i * g:(i + 1) * g, :]

    def rows(b):
        r = pl.ds(pl.multiple_of((pos[b] - start) * nkv, nkv), nkv)
        return (pltpu.make_async_copy(knew.at[b], ko.at[b, r], nsem.at[b, 0]),
                pltpu.make_async_copy(vnew.at[b], vo.at[b, r], nsem.at[b, 1]))

    def written(i, _):
        for cp in writes(i):
            cp.wait()
        b = i // nch
        p = pos[b] - start - i % nch * ch

        @pl.when(jnp.logical_and(p >= 0, p < ch))
        def _():
            for cp in rows(b):
                cp.start()

        return 0

    lax.fori_loop(0, total, written, 0)
    for b in range(nb):
        p = pos[b] - start

        @pl.when(jnp.logical_and(p >= 0, p < npos))
        def _():
            for cp in rows(b):
                cp.wait()


def combine(n, nb, ych, part, wo, y, wob, rbuf, xs, ybuf, wsem, ssem, rsem, ysem, zsem):
    me = lax.axis_index('sp')
    cols = wo.shape[1] // ych
    cps = []
    for c in range(ych):
        cp = pltpu.make_async_copy(wo.at[:, pl.ds(c * cols, cols)], wob.at[c], wsem.at[c])
        cp.start()
        cps.append(cp)
    greet(n)
    awaited(n)
    out = []
    for d in range(1, n):
        peer = lax.rem(me + d, n)
        cp = pltpu.make_async_remote_copy(
            src_ref=part.at[peer], dst_ref=rbuf.at[me], send_sem=ssem.at[d], recv_sem=rsem.at[d],
            device_id={'sp': peer}, device_id_type=MESH)
        cp.start()
        out.append(cp)
    rbuf[me] = part[me]
    for cp in out:
        cp.wait()
    o = rbuf[:, 0]
    ml = rbuf[:, 1]
    m = jnp.broadcast_to(ml[:, :, 0:1], o.shape)
    l = jnp.broadcast_to(ml[:, :, 64:65], o.shape)
    a = jnp.exp2(m - m.max(0)[None])
    out8 = (a * o).sum(0) / (a * l).sum(0)
    g = out8.shape[0] // nb
    dh = out8.shape[1]
    xs[...] = jnp.zeros_like(xs)
    for b in range(nb):
        for j in range(g):
            xs[b:b + 1, j * dh:(j + 1) * dh] = out8[b * g + j:b * g + j + 1]
    xl = xs[...].astype(bf16)
    sent = []
    for c in range(ych):
        cps[c].wait()
        ybuf[me, c] = jnp.dot(xl, wob[c], preferred_element_type=f32)[0:nb]
        for d in range(1, n):
            cp = pltpu.make_async_remote_copy(
                src_ref=ybuf.at[me, c], dst_ref=ybuf.at[me, c], send_sem=ysem.at[c, d], recv_sem=zsem.at[c, d],
                device_id={'sp': lax.rem(me + d, n)}, device_id_type=MESH)
            cp.start()
            sent.append(cp)
    for cp in sent:
        cp.wait()
    for c in range(ych):
        t = ybuf[0, c]
        for i in range(1, n):
            t = t + ybuf[i, c]
        y[:, c * cols:(c + 1) * cols] = t.astype(bf16)


def solution(mesh):
    n = mesh.shape['sp']

    def local(x, wq, wk, wv, wo, kc, vc, pos, lens):
        nb, npos, nkv, dh = kc.shape
        dm = x.shape[1]
        dq = wq.shape[1] // n
        dma = pltpu.SemaphoreType.DMA
        kc = kc.reshape(nb, npos * nkv, dh)
        vc = vc.reshape(nb, npos * nkv, dh)
        wch, ch, wide, slabs, kpre = 8, 512, 1024, 4, 8
        nch = npos // ch
        gat, kbuf, vbuf = pl.pallas_call(
            functools.partial(lookup, n, wch, ch, kpre),
            name='lookup',
            out_shape=(jax.ShapeDtypeStruct((n, nb, 8, dh), bf16), pltpu.VMEM(kc.shape, bf16), pltpu.VMEM(vc.shape, bf16)),
            in_specs=[ANY] * 6,
            out_specs=(VMEM,) * 3,
            scratch_shapes=[
                pltpu.VMEM(x.shape, bf16), pltpu.VMEM((dm, dq), bf16), pltpu.VMEM((dm, 2 * dh), bf16),
                pltpu.VMEM((nb, 8, dh), bf16), pltpu.VMEM((n, nb, 8, dh), bf16),
                dma, dma((2, wch)), dma((nb * nch,)), dma((nb * nch,)), dma((n,)), dma((n,))],
            compiler_params=pltpu.CompilerParams(collective_id=0, has_side_effects=True, vmem_limit_bytes=25 * MIB),
        )(*(pltpu.with_memory_space_constraint(t, pltpu.HBM) for t in (x, wq, wk, wv, kc, vc)))

        part, ko, vo = pl.pallas_call(
            functools.partial(attend, ch, wide, slabs),
            name='attend',
            out_shape=(jax.ShapeDtypeStruct((n, 2, 8, dh), f32), pltpu.HBM(kc.shape, bf16), pltpu.HBM(vc.shape, bf16)),
            in_specs=[ANY] * 2 + [VMEM] * 3,
            out_specs=(VMEM, ANY, ANY),
            scratch_shapes=[
                pltpu.SMEM((nb,), jnp.int32), pltpu.SMEM((nb,), jnp.int32),
                pltpu.VMEM((nb, npos * nkv // slabs, 128), f32), pltpu.VMEM((nb, slabs * dh, 128), bf16),
                pltpu.VMEM((nb, nkv, 128), f32), pltpu.VMEM((nb, nkv, 128), f32),
                pltpu.VMEM((nb, nkv, 128), f32), pltpu.VMEM((nb, nkv, 128), f32), pltpu.VMEM((nb, 128 // slabs, dh), f32),
                pltpu.VMEM((nb, nkv, dh), bf16), pltpu.VMEM((nb, nkv, dh), bf16),
                dma((2,)), dma((nb * nch,)), dma((nb * nch,)), dma((nb, 2))],
            compiler_params=pltpu.CompilerParams(vmem_limit_bytes=25 * MIB),
        )(*(pltpu.with_memory_space_constraint(t, pltpu.HBM) for t in (pos, lens)), gat, pltpu.with_memory_space_constraint(kbuf, pltpu.VMEM), pltpu.with_memory_space_constraint(vbuf, pltpu.VMEM))

        ych = 4
        cols = wo.shape[1] // ych
        y = pl.pallas_call(
            functools.partial(combine, n, nb, ych),
            name='combine',
            out_shape=jax.ShapeDtypeStruct((nb, wo.shape[1]), bf16),
            in_specs=[VMEM, ANY],
            out_specs=VMEM,
            scratch_shapes=[
                pltpu.VMEM((ych, wo.shape[0], cols), bf16), pltpu.VMEM((n, 2, 8, dh), f32), pltpu.VMEM((8, wo.shape[0]), f32),
                pltpu.VMEM((n, ych, nb, cols), f32),
                dma((ych,)), dma((n,)), dma((n,)), dma((ych, n)), dma((ych, n))],
            compiler_params=pltpu.CompilerParams(collective_id=1, has_side_effects=True, vmem_limit_bytes=8 * MIB),
        )(part, pltpu.with_memory_space_constraint(wo, pltpu.HBM))
        shape = (nb, npos, nkv, dh)
        return y, ko.reshape(shape), vo.reshape(shape)

    cache = P('dp', 'sp', None, None)
    return jax.shard_map(
        local, mesh=mesh,
        in_specs=(P('dp', None), P(None, None), P(None, None), P(None, None), P('sp', None),
                  cache, cache, P('dp'), P('dp')),
        out_specs=(P('dp', None), cache, cache),
        check_vma=False)
```

```python
import functools

import jax
import jax.numpy as jnp
from jax import lax
from jax.experimental import pallas as pl
from jax.experimental.pallas import tpu as pltpu
from jax.sharding import PartitionSpec as P

MESH = pl.DeviceIdType.MESH
ANY = pl.BlockSpec(memory_space=pl.ANY)
VMEM = pl.BlockSpec(memory_space=pltpu.VMEM)
SMEM = pl.BlockSpec(memory_space=pltpu.SMEM)
f32 = jnp.float32
bf16 = jnp.bfloat16
LOG2E = 1.4426950408889634
MIB = 1 << 20


def greet(n):
    me = lax.axis_index('sp')
    barrier = pltpu.get_barrier_semaphore()
    for d in range(1, n):
        pl.semaphore_signal(barrier, inc=1, device_id={'sp': lax.rem(me + d, n)}, device_id_type=MESH)


def awaited(n):
    pl.semaphore_wait(pltpu.get_barrier_semaphore(), n - 1)


def lookup(n, wch, ch, wide, slabs, early, kpre, pos_hbm, lens_hbm, x, wq, wk, wv, kc, vc, gat_out, kbuf, vbuf, sc, mrun, snew, qbd,
           pos, lens, xb, wqb, wab, send, gat, isem, xsem, wsem, ksem, vsem, ssem, rsem):
    me = lax.axis_index('sp')
    nb, dm = xb.shape
    dq, dh, da = wqb.shape[1], gat.shape[3], wab.shape[1]
    rows = dm // wch
    g = dq // dh
    nkv = n
    npos = kbuf.shape[1] // nkv
    nch = npos // ch
    total = nb * nch
    crow = ch * nkv
    srow = crow // slabs
    heads = 128 // slabs
    start = me * npos
    ninf = -jnp.inf

    def chunk(i):
        return i // nch, pl.ds(pl.multiple_of(i % nch * crow, crow), crow)

    def read_k(i):
        b, r = chunk(i)
        return pltpu.make_async_copy(kc.at[b, r], kbuf.at[b, r], ksem.at[i])

    def read_v(i):
        b, r = chunk(i)
        return pltpu.make_async_copy(vc.at[b, r], vbuf.at[b, r], vsem.at[i])

    xcp = pltpu.make_async_copy(x, xb, xsem)
    xcp.start()
    icps = [pltpu.make_async_copy(pos_hbm, pos, isem.at[0]), pltpu.make_async_copy(lens_hbm, lens, isem.at[1])]
    for cp in icps:
        cp.start()
    even = lax.rem(me, 2) == 0

    def read_q(c):
        r = pl.ds(c * rows, rows)
        return pltpu.make_async_copy(wq.at[r, pl.ds(pl.multiple_of(me * dq, 128), dq)], wqb.at[r], wsem.at[0, c])

    def read_a(w, c):
        r = pl.ds(c * rows, rows)
        return pltpu.make_async_copy(w.at[r, pl.ds(pl.multiple_of(me // 2 * da, 128), da)], wab.at[r], wsem.at[1, c])

    for c in range(wch):
        read_q(c).start()

    @pl.when(even)
    def _():
        for c in range(wch):
            read_a(wk, c).start()

    @pl.when(jnp.logical_not(even))
    def _():
        for c in range(wch):
            read_a(wv, c).start()

    for i in range(kpre):
        read_k(i).start()
    greet(n)
    xcp.wait()
    aq = jnp.zeros((nb, dq), f32)
    aa = jnp.zeros((nb, da), f32)
    for c in range(wch):
        read_q(c).wait()
        read_a(wk, c).wait()
        for i in range(kpre + c * (total - kpre) // wch, kpre + (c + 1) * (total - kpre) // wch):
            read_k(i).start()
        xc = xb[:, c * rows:(c + 1) * rows]
        r = pl.ds(c * rows, rows)
        aq += jnp.dot(xc, wqb[r, :], preferred_element_type=f32)
        aa += jnp.dot(xc, wab[r, :], preferred_element_type=f32)
    for b in range(nb):
        pieces = [aq[b:b + 1, i * dh:(i + 1) * dh] for i in range(g)] + [aa[b:b + 1, i * dh:(i + 1) * dh] for i in range(2)]
        pieces.append(jnp.zeros((8 - g - 2, dh), f32))
        tile = jnp.concatenate(pieces, axis=0).astype(bf16)
        send[b] = tile
        gat[me, b] = tile
    for i in range(early):
        read_v(i).start()
    awaited(n)
    out = []
    for d in range(1, n):
        cp = pltpu.make_async_remote_copy(
            src_ref=send, dst_ref=gat.at[me], send_sem=ssem.at[d], recv_sem=rsem.at[d],
            device_id={'sp': lax.rem(me + d, n)}, device_id_type=MESH)
        cp.start()
        out.append(cp)
    for cp in out:
        cp.wait()

    for cp in icps:
        cp.wait()
    gat_out[...] = gat[...]
    gf = gat[...].astype(f32)
    sub = lax.broadcasted_iota(jnp.int32, (nkv, 128), 0)
    lane = lax.broadcasted_iota(jnp.int32, (nkv, 128), 1)
    own = sub == (lane % heads) // g
    wrow = wide * nkv // slabs
    wch_n = npos // wide
    per = wide // ch
    first = jnp.where(own, lane // heads * (wide // slabs), 1 << 29)
    for b in range(nb):
        q = jnp.concatenate([gf[i, b, 0:g] for i in range(nkv)], axis=0)
        kn = jnp.concatenate([gf[i // 2 * 2, b, g + i % 2:g + i % 2 + 1] for i in range(nkv)], axis=0)
        zero = jnp.zeros_like(q)
        for s in range(slabs):
            a = jnp.concatenate([q if i == s else zero for i in range(slabs)], axis=0)
            qbd[b, s * dh:(s + 1) * dh, :] = a.T.astype(bf16)
        k16 = jnp.concatenate([kn, jnp.zeros_like(kn)], axis=0).astype(bf16)
        t = jnp.dot(k16, qbd[b, 0:dh, :], preferred_element_type=f32)[0:nkv]
        here = jnp.logical_and(pos[b] >= start, pos[b] < jnp.minimum(start + npos, lens[b]))
        limit = jnp.where(here, heads, 0)
        t = jnp.where(jnp.logical_and(own, lane < limit), t, ninf)
        snew[b] = t
        mrun[b] = t

    def scores(c, _):
        b = 0
        for t in range(per):
            read_k(c * per + t).wait()

        @pl.when(c * per + early < total)
        def _():
            for t in range(per):
                read_v(c * per + t + early).start()

        lim = jnp.minimum(pos[b], lens[b]) - start - c * wide
        acc = None
        for s in range(0, slabs, 2):
            k2 = jnp.concatenate(
                [kbuf[b, pl.ds(pl.multiple_of((c * slabs + s + t) * wrow, wrow), wrow), :] for t in range(2)], axis=1)
            t = jnp.dot(k2, qbd[b, s * dh:(s + 2) * dh, :], preferred_element_type=f32)
            acc = t if acc is None else acc + t
        acc = acc.reshape(wrow // nkv, nkv, 128)
        left = lim - lax.broadcasted_iota(jnp.int32, acc.shape, 0)
        t = jnp.where(first[None] < left, acc, ninf)
        sc[pl.ds(pl.multiple_of(c * wrow, wrow), wrow), :] = t.reshape(wrow, 128)
        mrun[b] = jnp.maximum(mrun[b], t.max(0))
        return 0

    lax.fori_loop(0, wch_n, scores, 0)
    for i in range(nch, total):
        read_k(i).wait()

    def landed(i, _):
        read_v(i).wait()
        return 0

    lax.fori_loop(0, total, landed, 0)


def attend(ch, wide, slabs, pos_hbm, lens_hbm, gat, kbuf, vbuf, sc, mrun, snew, qbd, part, ko, vo, pos, lens, rest, mall, lrun, orun, knew, vnew,
           isem, ksem, vsem, nsem):
    me = lax.axis_index('sp')
    nkv, nb, _, dh = gat.shape
    npos = kbuf.shape[1] // nkv
    nch = npos // ch
    total = nb * nch
    crow = ch * nkv
    srow = crow // slabs
    heads = 128 // slabs
    g = heads // nkv
    start = me * npos
    scale = dh ** -0.5 * LOG2E
    ninf = -jnp.inf

    icps = [pltpu.make_async_copy(pos_hbm, pos, isem.at[0]), pltpu.make_async_copy(lens_hbm, lens, isem.at[1])]
    for cp in icps:
        cp.start()

    def writes(i):
        b, r = i // nch, pl.ds(pl.multiple_of(i % nch * crow, crow), crow)
        return (pltpu.make_async_copy(kbuf.at[b, r], ko.at[b, r], ksem.at[i]),
                pltpu.make_async_copy(vbuf.at[b, r], vo.at[b, r], vsem.at[i]))

    def begin(i, _):
        for t, cp in enumerate(writes(i)):
            cp.start(priority=t)
        return 0

    lax.fori_loop(0, total, begin, 0)

    gf = gat[...].astype(f32)
    lrun[...] = jnp.zeros_like(lrun)
    orun[...] = jnp.zeros_like(orun)
    for b in range(nb):
        knew[b] = jnp.concatenate([gf[i // 2 * 2, b, g + i % 2:g + i % 2 + 1] for i in range(nkv)], axis=0).astype(bf16)
        vnew[b] = jnp.concatenate([gf[i // 2 * 2 + 1, b, g + i % 2:g + i % 2 + 1] for i in range(nkv)], axis=0).astype(bf16)
        mall[b] = mrun[b]

    wrow = wide * nkv // slabs
    wch_n = npos // wide

    sub = lax.broadcasted_iota(jnp.int32, (nkv, 128), 0)
    lane = lax.broadcasted_iota(jnp.int32, (nkv, 128), 1)
    own = sub == (lane % heads) // g
    first = jnp.where(own, lane // heads * (wide // slabs), 1 << 29)

    def settle(b):
        m = jnp.broadcast_to(mall[b].max(0, keepdims=True), (nkv, 128))
        k = heads
        while k < 128:
            m = jnp.maximum(m, pltpu.roll(m, k, 1))
            k *= 2
        mall[b] = m

    def mix(b, scored, c):
        lim = jnp.minimum(pos[b], lens[b]) - start - c * wide

        @pl.when(lim > 0)
        def _():
            m = mall[b]
            m = jnp.where(m == ninf, 0.0, m)
            t = scored[pl.ds(pl.multiple_of(c * wrow, wrow), wrow), :].reshape(wrow // nkv, nkv, 128)
            e = jnp.exp2((t - m[None]) * scale)
            lrun[b] += e.sum(0)
            et = e.reshape(wrow, 128).astype(bf16).T
            o = orun[b]
            for s in range(slabs):
                v = vbuf[b, pl.ds(pl.multiple_of((c * slabs + s) * wrow, wrow), wrow), :]
                o += jnp.dot(et[s * heads:(s + 1) * heads], v, preferred_element_type=f32)
            orun[b] = o

    def scores(b, scored, c):
        lim = jnp.minimum(pos[b], lens[b]) - start - c * wide

        @pl.when(lim > 0)
        def _():
            acc = None
            for s in range(0, slabs, 2):
                k2 = jnp.concatenate(
                    [kbuf[b, pl.ds(pl.multiple_of((c * slabs + s + t) * wrow, wrow), wrow), :] for t in range(2)], axis=1)
                t = jnp.dot(k2, qbd[b, s * dh:(s + 2) * dh, :], preferred_element_type=f32)
                acc = t if acc is None else acc + t
            acc = acc.reshape(wrow // nkv, nkv, 128)
            left = lim - lax.broadcasted_iota(jnp.int32, acc.shape, 0)
            t = jnp.where(first[None] < left, acc, ninf)
            scored[pl.ds(pl.multiple_of(c * wrow, wrow), wrow), :] = t.reshape(wrow, 128)
            mall[b] = jnp.maximum(mall[b], t.max(0))

    def loop(step, b, scored):
        def body(c, _):
            step(b, scored, c)
            return 0

        lax.fori_loop(0, wch_n, body, 0)

    for cp in icps:
        cp.wait()
    settle(0)
    loop(mix, 0, sc)
    for b in range(1, nb):
        loop(scores, b, rest)
        settle(b)
        loop(mix, b, rest)

    half = lax.broadcasted_iota(jnp.int32, (heads, 128), 1) < 64
    for b in range(nb):
        m = mall[b]
        e = jnp.exp2((snew[b] - jnp.where(m == ninf, 0.0, m)) * scale)
        pad = jnp.zeros_like(e)
        e16 = jnp.concatenate([e, pad], axis=0).astype(bf16)
        v16 = jnp.concatenate([vnew[b].astype(f32), pad], axis=0).astype(bf16)
        o = orun[b] + lax.dot_general(e16, v16, (((0,), (0,)), ((), ())), preferred_element_type=f32)[0:heads]
        l = jnp.broadcast_to((lrun[b] + e).sum(0, keepdims=True), (nkv, 128))
        k = heads
        while k < 128:
            l = l + pltpu.roll(l, k, 1)
            k *= 2
        lt = jnp.broadcast_to(l[0:1], (128, 128)).T[0:heads]
        mt = jnp.broadcast_to(m[0:1] * scale, (128, 128)).T[0:heads]
        ml = jnp.where(half, mt, lt)
        for i in range(nkv):
            part[i, 0, b * g:(b + 1) * g, :] = o[i * g:(i + 1) * g, :]
            part[i, 1, b * g:(b + 1) * g, :] = ml[i * g:(i + 1) * g, :]

    def rows(b):
        r = pl.ds(pl.multiple_of((pos[b] - start) * nkv, nkv), nkv)
        return (pltpu.make_async_copy(knew.at[b], ko.at[b, r], nsem.at[b, 0]),
                pltpu.make_async_copy(vnew.at[b], vo.at[b, r], nsem.at[b, 1]))

    def written(i, _):
        for cp in writes(i):
            cp.wait()
        b = i // nch
        p = pos[b] - start - i % nch * ch

        @pl.when(jnp.logical_and(p >= 0, p < ch))
        def _():
            for cp in rows(b):
                cp.start()

        return 0

    lax.fori_loop(0, total, written, 0)
    for b in range(nb):
        p = pos[b] - start

        @pl.when(jnp.logical_and(p >= 0, p < npos))
        def _():
            for cp in rows(b):
                cp.wait()


def combine(n, nb, ych, part, wo, y, wob, rbuf, xs, ybuf, wsem, ssem, rsem, ysem, zsem):
    me = lax.axis_index('sp')
    cols = wo.shape[1] // ych
    cps = []
    for c in range(ych):
        cp = pltpu.make_async_copy(wo.at[:, pl.ds(c * cols, cols)], wob.at[c], wsem.at[c])
        cp.start()
        cps.append(cp)
    greet(n)
    awaited(n)
    out = []
    for d in range(1, n):
        peer = lax.rem(me + d, n)
        cp = pltpu.make_async_remote_copy(
            src_ref=part.at[peer], dst_ref=rbuf.at[me], send_sem=ssem.at[d], recv_sem=rsem.at[d],
            device_id={'sp': peer}, device_id_type=MESH)
        cp.start()
        out.append(cp)
    rbuf[me] = part[me]
    for cp in out:
        cp.wait()
    o = rbuf[:, 0]
    ml = rbuf[:, 1]
    m = jnp.broadcast_to(ml[:, :, 0:1], o.shape)
    l = jnp.broadcast_to(ml[:, :, 64:65], o.shape)
    a = jnp.exp2(m - m.max(0)[None])
    out8 = (a * o).sum(0) / (a * l).sum(0)
    g = out8.shape[0] // nb
    dh = out8.shape[1]
    xs[...] = jnp.zeros_like(xs)
    for b in range(nb):
        for j in range(g):
            xs[b:b + 1, j * dh:(j + 1) * dh] = out8[b * g + j:b * g + j + 1]
    xl = xs[...].astype(bf16)
    sent = []
    for c in range(ych):
        cps[c].wait()
        ybuf[me, c] = jnp.dot(xl, wob[c], preferred_element_type=f32)[0:nb]
        for d in range(1, n):
            cp = pltpu.make_async_remote_copy(
                src_ref=ybuf.at[me, c], dst_ref=ybuf.at[me, c], send_sem=ysem.at[c, d], recv_sem=zsem.at[c, d],
                device_id={'sp': lax.rem(me + d, n)}, device_id_type=MESH)
            cp.start()
            sent.append(cp)
    for cp in sent:
        cp.wait()
    for c in range(ych):
        t = ybuf[0, c]
        for i in range(1, n):
            t = t + ybuf[i, c]
        y[:, c * cols:(c + 1) * cols] = t.astype(bf16)


def solution(mesh):
    n = mesh.shape['sp']

    def local(x, wq, wk, wv, wo, kc, vc, pos, lens):
        nb, npos, nkv, dh = kc.shape
        dm = x.shape[1]
        dq = wq.shape[1] // n
        dma = pltpu.SemaphoreType.DMA
        kc = kc.reshape(nb, npos * nkv, dh)
        vc = vc.reshape(nb, npos * nkv, dh)
        wch, ch, wide, slabs, early, kpre = 8, 512, 1024, 4, 8, 2
        nch = npos // ch
        small = jax.ShapeDtypeStruct((nb, nkv, 128), f32)
        gat, kbuf, vbuf, sc, mrun, snew, qbd = pl.pallas_call(
            functools.partial(lookup, n, wch, ch, wide, slabs, early, kpre),
            name='lookup',
            out_shape=(jax.ShapeDtypeStruct((n, nb, 8, dh), bf16), pltpu.VMEM(kc.shape, bf16), pltpu.VMEM(vc.shape, bf16),
                       pltpu.VMEM((npos * nkv // slabs, 128), f32), small, small,
                       jax.ShapeDtypeStruct((nb, slabs * dh, 128), bf16)),
            in_specs=[ANY] * 8,
            out_specs=(VMEM,) * 7,
            scratch_shapes=[
                pltpu.SMEM((nb,), jnp.int32), pltpu.SMEM((nb,), jnp.int32),
                pltpu.VMEM(x.shape, bf16), pltpu.VMEM((dm, dq), bf16), pltpu.VMEM((dm, 2 * dh), bf16),
                pltpu.VMEM((nb, 8, dh), bf16), pltpu.VMEM((n, nb, 8, dh), bf16),
                dma((2,)), dma, dma((2, wch)), dma((nb * nch,)), dma((nb * nch,)), dma((n,)), dma((n,))],
            compiler_params=pltpu.CompilerParams(collective_id=0, has_side_effects=True, vmem_limit_bytes=12 * MIB),
        )(*(pltpu.with_memory_space_constraint(t, pltpu.HBM) for t in (pos, lens, x, wq, wk, wv, kc, vc)))

        part, ko, vo = pl.pallas_call(
            functools.partial(attend, ch, wide, slabs),
            name='attend',
            out_shape=(jax.ShapeDtypeStruct((n, 2, 8, dh), f32), pltpu.HBM(kc.shape, bf16), pltpu.HBM(vc.shape, bf16)),
            in_specs=[ANY] * 2 + [VMEM] * 7,
            out_specs=(VMEM, ANY, ANY),
            scratch_shapes=[
                pltpu.SMEM((nb,), jnp.int32), pltpu.SMEM((nb,), jnp.int32), pltpu.VMEM((npos * nkv // slabs, 128), f32),
                pltpu.VMEM((nb, nkv, 128), f32), pltpu.VMEM((nb, nkv, 128), f32), pltpu.VMEM((nb, 128 // slabs, dh), f32),
                pltpu.VMEM((nb, nkv, dh), bf16), pltpu.VMEM((nb, nkv, dh), bf16),
                dma((2,)), dma((nb * nch,)), dma((nb * nch,)), dma((nb, 2))],
            compiler_params=pltpu.CompilerParams(vmem_limit_bytes=12 * MIB),
        )(*(pltpu.with_memory_space_constraint(t, pltpu.HBM) for t in (pos, lens)), gat, kbuf, vbuf, sc, mrun, snew, qbd)

        ych = 4
        cols = wo.shape[1] // ych
        y = pl.pallas_call(
            functools.partial(combine, n, nb, ych),
            name='combine',
            out_shape=jax.ShapeDtypeStruct((nb, wo.shape[1]), bf16),
            in_specs=[VMEM, ANY],
            out_specs=VMEM,
            scratch_shapes=[
                pltpu.VMEM((ych, wo.shape[0], cols), bf16), pltpu.VMEM((n, 2, 8, dh), f32), pltpu.VMEM((8, wo.shape[0]), f32),
                pltpu.VMEM((n, ych, nb, cols), f32),
                dma((ych,)), dma((n,)), dma((n,)), dma((ych, n)), dma((ych, n))],
            compiler_params=pltpu.CompilerParams(collective_id=1, has_side_effects=True, vmem_limit_bytes=8 * MIB),
        )(part, pltpu.with_memory_space_constraint(wo, pltpu.HBM))
        shape = (nb, npos, nkv, dh)
        return y, ko.reshape(shape), vo.reshape(shape)

    cache = P('dp', 'sp', None, None)
    return jax.shard_map(
        local, mesh=mesh,
        in_specs=(P('dp', None), P(None, None), P(None, None), P(None, None), P('sp', None),
                  cache, cache, P('dp'), P('dp')),
        out_specs=(P('dp', None), cache, cache),
        check_vma=False)
```

```python
import functools

import jax
import jax.numpy as jnp
from jax import lax
from jax.experimental import pallas as pl
from jax.experimental.pallas import tpu as pltpu
from jax.sharding import PartitionSpec as P

MESH = pl.DeviceIdType.MESH
ANY = pl.BlockSpec(memory_space=pl.ANY)
VMEM = pl.BlockSpec(memory_space=pltpu.VMEM)
SMEM = pl.BlockSpec(memory_space=pltpu.SMEM)
f32 = jnp.float32
bf16 = jnp.bfloat16
LOG2E = 1.4426950408889634
MIB = 1 << 20


def greet(n):
    me = lax.axis_index('sp')
    barrier = pltpu.get_barrier_semaphore()
    for d in range(1, n):
        pl.semaphore_signal(barrier, inc=1, device_id={'sp': lax.rem(me + d, n)}, device_id_type=MESH)


def awaited(n):
    pl.semaphore_wait(pltpu.get_barrier_semaphore(), n - 1)


def lookup(n, wch, ch, wide, slabs, early, kpre, pos_hbm, lens_hbm, x, wq, wk, wv, kc, vc, gat_out, kbuf, vbuf, sc, mrun, snew, qbd,
           pos, lens, xb, wqb, wab, send, gat, isem, xsem, wsem, ksem, vsem, ssem, rsem):
    me = lax.axis_index('sp')
    nb, dm = xb.shape
    dq, dh, da = wqb.shape[1], gat.shape[3], wab.shape[1]
    rows = dm // wch
    g = dq // dh
    nkv = n
    npos = kbuf.shape[1] // nkv
    nch = npos // ch
    total = nb * nch
    crow = ch * nkv
    srow = crow // slabs
    heads = 128 // slabs
    start = me * npos
    ninf = -jnp.inf

    def chunk(i):
        return i // nch, pl.ds(pl.multiple_of(i % nch * crow, crow), crow)

    def read_k(i):
        b, r = chunk(i)
        return pltpu.make_async_copy(kc.at[b, r], kbuf.at[b, r], ksem.at[i])

    def read_v(i):
        b, r = chunk(i)
        return pltpu.make_async_copy(vc.at[b, r], vbuf.at[b, r], vsem.at[i])

    xcp = pltpu.make_async_copy(x, xb, xsem)
    xcp.start()
    icps = [pltpu.make_async_copy(pos_hbm, pos, isem.at[0]), pltpu.make_async_copy(lens_hbm, lens, isem.at[1])]
    for cp in icps:
        cp.start()
    even = lax.rem(me, 2) == 0

    def read_q(c):
        r = pl.ds(c * rows, rows)
        return pltpu.make_async_copy(wq.at[r, pl.ds(pl.multiple_of(me * dq, 128), dq)], wqb.at[r], wsem.at[0, c])

    def read_a(w, c):
        r = pl.ds(c * rows, rows)
        return pltpu.make_async_copy(w.at[r, pl.ds(pl.multiple_of(me // 2 * da, 128), da)], wab.at[r], wsem.at[1, c])

    for c in range(wch):
        read_q(c).start()

    @pl.when(even)
    def _():
        for c in range(wch):
            read_a(wk, c).start()

    @pl.when(jnp.logical_not(even))
    def _():
        for c in range(wch):
            read_a(wv, c).start()

    for i in range(kpre):
        read_k(i).start()
    greet(n)
    xcp.wait()
    aq = jnp.zeros((nb, dq), f32)
    aa = jnp.zeros((nb, da), f32)
    for c in range(wch):
        read_q(c).wait()
        read_a(wk, c).wait()
        for i in range(kpre + c * (total - kpre) // wch, kpre + (c + 1) * (total - kpre) // wch):
            read_k(i).start()
        xc = xb[:, c * rows:(c + 1) * rows]
        r = pl.ds(c * rows, rows)
        aq += jnp.dot(xc, wqb[r, :], preferred_element_type=f32)
        aa += jnp.dot(xc, wab[r, :], preferred_element_type=f32)
    for b in range(nb):
        pieces = [aq[b:b + 1, i * dh:(i + 1) * dh] for i in range(g)] + [aa[b:b + 1, i * dh:(i + 1) * dh] for i in range(2)]
        pieces.append(jnp.zeros((8 - g - 2, dh), f32))
        tile = jnp.concatenate(pieces, axis=0).astype(bf16)
        send[b] = tile
        gat[me, b] = tile
    for i in range(early):
        read_v(i).start()
    awaited(n)
    out = []
    for d in range(1, n):
        cp = pltpu.make_async_remote_copy(
            src_ref=send, dst_ref=gat.at[me], send_sem=ssem.at[d], recv_sem=rsem.at[d],
            device_id={'sp': lax.rem(me + d, n)}, device_id_type=MESH)
        cp.start()
        out.append(cp)
    for cp in out:
        cp.wait()

    for cp in icps:
        cp.wait()
    gat_out[...] = gat[...]
    gf = gat[...].astype(f32)
    sub = lax.broadcasted_iota(jnp.int32, (nkv, 128), 0)
    lane = lax.broadcasted_iota(jnp.int32, (nkv, 128), 1)
    own = sub == (lane % heads) // g
    wrow = wide * nkv // slabs
    wch_n = npos // wide
    per = wide // ch
    first = jnp.where(own, lane // heads * (wide // slabs), 1 << 29)
    for b in range(nb):
        q = jnp.concatenate([gf[i, b, 0:g] for i in range(nkv)], axis=0)
        kn = jnp.concatenate([gf[i // 2 * 2, b, g + i % 2:g + i % 2 + 1] for i in range(nkv)], axis=0)
        zero = jnp.zeros_like(q)
        for s in range(slabs):
            a = jnp.concatenate([q if i == s else zero for i in range(slabs)], axis=0)
            qbd[b, s * dh:(s + 1) * dh, :] = a.T.astype(bf16)
        k16 = jnp.concatenate([kn, jnp.zeros_like(kn)], axis=0).astype(bf16)
        t = jnp.dot(k16, qbd[b, 0:dh, :], preferred_element_type=f32)[0:nkv]
        here = jnp.logical_and(pos[b] >= start, pos[b] < jnp.minimum(start + npos, lens[b]))
        limit = jnp.where(here, heads, 0)
        t = jnp.where(jnp.logical_and(own, lane < limit), t, ninf)
        snew[b] = t
        mrun[b] = t

    def scores(c, _):
        b = 0
        for t in range(per):
            read_k(c * per + t).wait()

        @pl.when(c * per + early < total)
        def _():
            for t in range(per):
                read_v(c * per + t + early).start()

        lim = jnp.minimum(pos[b], lens[b]) - start - c * wide
        acc = None
        for s in range(0, slabs, 2):
            k2 = jnp.concatenate(
                [kbuf[b, pl.ds(pl.multiple_of((c * slabs + s + t) * wrow, wrow), wrow), :] for t in range(2)], axis=1)
            t = jnp.dot(k2, qbd[b, s * dh:(s + 2) * dh, :], preferred_element_type=f32)
            acc = t if acc is None else acc + t
        acc = acc.reshape(wrow // nkv, nkv, 128)
        left = lim - lax.broadcasted_iota(jnp.int32, acc.shape, 0)
        t = jnp.where(first[None] < left, acc, ninf)
        sc[pl.ds(pl.multiple_of(c * wrow, wrow), wrow), :] = t.reshape(wrow, 128)
        mrun[b] = jnp.maximum(mrun[b], t.max(0))
        return 0

    lax.fori_loop(0, wch_n, scores, 0)
    for i in range(nch, total):
        read_k(i).wait()

    def landed(i, _):
        read_v(i).wait()
        return 0

    lax.fori_loop(0, total, landed, 0)


def attend(ch, wide, slabs, pos_hbm, lens_hbm, gat, kbuf, vbuf, sc, mrun, snew, qbd, part, ko, vo, pos, lens, rest, mall, lrun, orun, knew, vnew,
           isem, ksem, vsem, nsem):
    me = lax.axis_index('sp')
    nkv, nb, _, dh = gat.shape
    npos = kbuf.shape[1] // nkv
    nch = npos // ch
    total = nb * nch
    crow = ch * nkv
    srow = crow // slabs
    heads = 128 // slabs
    g = heads // nkv
    start = me * npos
    scale = dh ** -0.5 * LOG2E
    ninf = -jnp.inf

    icps = [pltpu.make_async_copy(pos_hbm, pos, isem.at[0]), pltpu.make_async_copy(lens_hbm, lens, isem.at[1])]
    for cp in icps:
        cp.start()

    def writes(i):
        b, r = i // nch, pl.ds(pl.multiple_of(i % nch * crow, crow), crow)
        return (pltpu.make_async_copy(kbuf.at[b, r], ko.at[b, r], ksem.at[i]),
                pltpu.make_async_copy(vbuf.at[b, r], vo.at[b, r], vsem.at[i]))

    def begin(i, _):
        for t, cp in enumerate(writes(i)):
            cp.start(priority=t)
        return 0

    lax.fori_loop(0, total, begin, 0)

    gf = gat[...].astype(f32)
    lrun[...] = jnp.zeros_like(lrun)
    orun[...] = jnp.zeros_like(orun)
    for b in range(nb):
        knew[b] = jnp.concatenate([gf[i // 2 * 2, b, g + i % 2:g + i % 2 + 1] for i in range(nkv)], axis=0).astype(bf16)
        vnew[b] = jnp.concatenate([gf[i // 2 * 2 + 1, b, g + i % 2:g + i % 2 + 1] for i in range(nkv)], axis=0).astype(bf16)
        mall[b] = mrun[b]

    wrow = wide * nkv // slabs
    wch_n = npos // wide

    sub = lax.broadcasted_iota(jnp.int32, (nkv, 128), 0)
    lane = lax.broadcasted_iota(jnp.int32, (nkv, 128), 1)
    own = sub == (lane % heads) // g
    first = jnp.where(own, lane // heads * (wide // slabs), 1 << 29)

    def settle(b):
        m = jnp.broadcast_to(mall[b].max(0, keepdims=True), (nkv, 128))
        k = heads
        while k < 128:
            m = jnp.maximum(m, pltpu.roll(m, k, 1))
            k *= 2
        mall[b] = m

    def mix(b, scored, c):
        lim = jnp.minimum(pos[b], lens[b]) - start - c * wide

        @pl.when(lim > 0)
        def _():
            m = mall[b]
            m = jnp.where(m == ninf, 0.0, m)
            t = scored[pl.ds(pl.multiple_of(c * wrow, wrow), wrow), :].reshape(wrow // nkv, nkv, 128)
            e = jnp.exp2((t - m[None]) * scale)
            lrun[b] += e.sum(0)
            et = e.reshape(wrow, 128).astype(bf16).T
            o = orun[b]
            for s in range(slabs):
                v = vbuf[b, pl.ds(pl.multiple_of((c * slabs + s) * wrow, wrow), wrow), :]
                o += jnp.dot(et[s * heads:(s + 1) * heads], v, preferred_element_type=f32)
            orun[b] = o

    def scores(b, scored, c):
        lim = jnp.minimum(pos[b], lens[b]) - start - c * wide

        @pl.when(lim > 0)
        def _():
            acc = None
            for s in range(0, slabs, 2):
                k2 = jnp.concatenate(
                    [kbuf[b, pl.ds(pl.multiple_of((c * slabs + s + t) * wrow, wrow), wrow), :] for t in range(2)], axis=1)
                t = jnp.dot(k2, qbd[b, s * dh:(s + 2) * dh, :], preferred_element_type=f32)
                acc = t if acc is None else acc + t
            acc = acc.reshape(wrow // nkv, nkv, 128)
            left = lim - lax.broadcasted_iota(jnp.int32, acc.shape, 0)
            t = jnp.where(first[None] < left, acc, ninf)
            scored[pl.ds(pl.multiple_of(c * wrow, wrow), wrow), :] = t.reshape(wrow, 128)
            mall[b] = jnp.maximum(mall[b], t.max(0))

    def loop(step, b, scored):
        def body(c, _):
            step(b, scored, c)
            return 0

        lax.fori_loop(0, wch_n, body, 0)

    for cp in icps:
        cp.wait()
    settle(0)
    loop(mix, 0, sc)
    for b in range(1, nb):
        loop(scores, b, rest)
        settle(b)
        loop(mix, b, rest)

    half = lax.broadcasted_iota(jnp.int32, (heads, 128), 1) < 64
    for b in range(nb):
        m = mall[b]
        e = jnp.exp2((snew[b] - jnp.where(m == ninf, 0.0, m)) * scale)
        pad = jnp.zeros_like(e)
        e16 = jnp.concatenate([e, pad], axis=0).astype(bf16)
        v16 = jnp.concatenate([vnew[b].astype(f32), pad], axis=0).astype(bf16)
        o = orun[b] + lax.dot_general(e16, v16, (((0,), (0,)), ((), ())), preferred_element_type=f32)[0:heads]
        l = jnp.broadcast_to((lrun[b] + e).sum(0, keepdims=True), (nkv, 128))
        k = heads
        while k < 128:
            l = l + pltpu.roll(l, k, 1)
            k *= 2
        lt = jnp.broadcast_to(l[0:1], (128, 128)).T[0:heads]
        mt = jnp.broadcast_to(m[0:1] * scale, (128, 128)).T[0:heads]
        ml = jnp.where(half, mt, lt)
        for i in range(nkv):
            part[i, 0, b * g:(b + 1) * g, :] = o[i * g:(i + 1) * g, :]
            part[i, 1, b * g:(b + 1) * g, :] = ml[i * g:(i + 1) * g, :]

    def rows(b):
        r = pl.ds(pl.multiple_of((pos[b] - start) * nkv, nkv), nkv)
        return (pltpu.make_async_copy(knew.at[b], ko.at[b, r], nsem.at[b, 0]),
                pltpu.make_async_copy(vnew.at[b], vo.at[b, r], nsem.at[b, 1]))

    def written(i, _):
        for cp in writes(i):
            cp.wait()
        b = i // nch
        p = pos[b] - start - i % nch * ch

        @pl.when(jnp.logical_and(p >= 0, p < ch))
        def _():
            for cp in rows(b):
                cp.start()

        return 0

    lax.fori_loop(0, total, written, 0)
    for b in range(nb):
        p = pos[b] - start

        @pl.when(jnp.logical_and(p >= 0, p < npos))
        def _():
            for cp in rows(b):
                cp.wait()


def combine(n, nb, ych, part, wo, y, wob, rbuf, xs, mine, far, half, twin, wsem, ssem, rsem, ysem, zsem, hsem, tsem):
    me = lax.axis_index('sp')
    cols = wo.shape[1] // ych
    cps = []
    for c in range(ych):
        cp = pltpu.make_async_copy(wo.at[:, pl.ds(c * cols, cols)], wob.at[c], wsem.at[c])
        cp.start()
        cps.append(cp)
    greet(n)
    awaited(n)
    out = []
    for d in range(1, n):
        peer = lax.rem(me + d, n)
        cp = pltpu.make_async_remote_copy(
            src_ref=part.at[peer], dst_ref=rbuf.at[me], send_sem=ssem.at[d], recv_sem=rsem.at[d],
            device_id={'sp': peer}, device_id_type=MESH)
        cp.start()
        out.append(cp)
    rbuf[me] = part[me]
    for cp in out:
        cp.wait()
    o = rbuf[:, 0]
    ml = rbuf[:, 1]
    m = jnp.broadcast_to(ml[:, :, 0:1], o.shape)
    l = jnp.broadcast_to(ml[:, :, 64:65], o.shape)
    a = jnp.exp2(m - m.max(0)[None])
    out8 = (a * o).sum(0) / (a * l).sum(0)
    g = out8.shape[0] // nb
    dh = out8.shape[1]
    xs[...] = jnp.zeros_like(xs)
    for b in range(nb):
        for j in range(g):
            xs[b:b + 1, j * dh:(j + 1) * dh] = out8[b * g + j:b * g + j + 1]
    xl = xs[...].astype(bf16)
    over_x = me + 2 - 4 * lax.rem(me // 2, 2)
    over_y = me + 4 - 8 * (me // 4)
    sent = []
    for c in range(ych):
        cps[c].wait()
        mine[c] = jnp.dot(xl, wob[c], preferred_element_type=f32)[0:nb]
        for j, peer in enumerate((over_x, over_y, over_x + over_y - me)):
            cp = pltpu.make_async_remote_copy(
                src_ref=mine.at[c], dst_ref=far.at[j, c], send_sem=ysem.at[c, j], recv_sem=zsem.at[c, j],
                device_id={'sp': peer}, device_id_type=MESH)
            cp.start()
            sent.append(cp)
    swaps = []
    for c in range(ych):
        for j in range(3):
            sent[3 * c + j].wait()
        half[c] = (mine[c] + far[0, c]) + (far[1, c] + far[2, c])
        cp = pltpu.make_async_remote_copy(
            src_ref=half.at[c], dst_ref=twin.at[c], send_sem=hsem.at[c], recv_sem=tsem.at[c],
            device_id={'sp': me + 1 - 2 * lax.rem(me, 2)}, device_id_type=MESH)
        cp.start()
        swaps.append(cp)
    for c in range(ych):
        swaps[c].wait()
        y[:, c * cols:(c + 1) * cols] = (half[c] + twin[c]).astype(bf16)


def solution(mesh):
    n = mesh.shape['sp']

    def local(x, wq, wk, wv, wo, kc, vc, pos, lens):
        nb, npos, nkv, dh = kc.shape
        dm = x.shape[1]
        dq = wq.shape[1] // n
        dma = pltpu.SemaphoreType.DMA
        kc = kc.reshape(nb, npos * nkv, dh)
        vc = vc.reshape(nb, npos * nkv, dh)
        wch, ch, wide, slabs, early, kpre = 8, 1024, 1024, 4, 4, 1
        nch = npos // ch
        small = jax.ShapeDtypeStruct((nb, nkv, 128), f32)
        gat, kbuf, vbuf, sc, mrun, snew, qbd = pl.pallas_call(
            functools.partial(lookup, n, wch, ch, wide, slabs, early, kpre),
            name='lookup',
            out_shape=(jax.ShapeDtypeStruct((n, nb, 8, dh), bf16), pltpu.VMEM(kc.shape, bf16), pltpu.VMEM(vc.shape, bf16),
                       pltpu.VMEM((npos * nkv // slabs, 128), f32), small, small,
                       jax.ShapeDtypeStruct((nb, slabs * dh, 128), bf16)),
            in_specs=[ANY] * 8,
            out_specs=(VMEM,) * 7,
            scratch_shapes=[
                pltpu.SMEM((nb,), jnp.int32), pltpu.SMEM((nb,), jnp.int32),
                pltpu.VMEM(x.shape, bf16), pltpu.VMEM((dm, dq), bf16), pltpu.VMEM((dm, 2 * dh), bf16),
                pltpu.VMEM((nb, 8, dh), bf16), pltpu.VMEM((n, nb, 8, dh), bf16),
                dma((2,)), dma, dma((2, wch)), dma((nb * nch,)), dma((nb * nch,)), dma((n,)), dma((n,))],
            compiler_params=pltpu.CompilerParams(collective_id=0, has_side_effects=True, vmem_limit_bytes=12 * MIB),
        )(*(pltpu.with_memory_space_constraint(t, pltpu.HBM) for t in (pos, lens, x, wq, wk, wv, kc, vc)))

        part, ko, vo = pl.pallas_call(
            functools.partial(attend, ch, wide, slabs),
            name='attend',
            out_shape=(jax.ShapeDtypeStruct((n, 2, 8, dh), f32), pltpu.HBM(kc.shape, bf16), pltpu.HBM(vc.shape, bf16)),
            in_specs=[ANY] * 2 + [VMEM] * 7,
            out_specs=(VMEM, ANY, ANY),
            scratch_shapes=[
                pltpu.SMEM((nb,), jnp.int32), pltpu.SMEM((nb,), jnp.int32), pltpu.VMEM((npos * nkv // slabs, 128), f32),
                pltpu.VMEM((nb, nkv, 128), f32), pltpu.VMEM((nb, nkv, 128), f32), pltpu.VMEM((nb, 128 // slabs, dh), f32),
                pltpu.VMEM((nb, nkv, dh), bf16), pltpu.VMEM((nb, nkv, dh), bf16),
                dma((2,)), dma((nb * nch,)), dma((nb * nch,)), dma((nb, 2))],
            compiler_params=pltpu.CompilerParams(vmem_limit_bytes=12 * MIB),
        )(*(pltpu.with_memory_space_constraint(t, pltpu.HBM) for t in (pos, lens)), gat, kbuf, vbuf, sc, mrun, snew, qbd)

        ych = 4
        cols = wo.shape[1] // ych
        y = pl.pallas_call(
            functools.partial(combine, n, nb, ych),
            name='combine',
            out_shape=jax.ShapeDtypeStruct((nb, wo.shape[1]), bf16),
            in_specs=[VMEM, ANY],
            out_specs=VMEM,
            scratch_shapes=[
                pltpu.VMEM((ych, wo.shape[0], cols), bf16), pltpu.VMEM((n, 2, 8, dh), f32), pltpu.VMEM((8, wo.shape[0]), f32),
                pltpu.VMEM((ych, nb, cols), f32), pltpu.VMEM((3, ych, nb, cols), f32),
                pltpu.VMEM((ych, nb, cols), f32), pltpu.VMEM((ych, nb, cols), f32),
                dma((ych,)), dma((n,)), dma((n,)), dma((ych, 3)), dma((ych, 3)), dma((ych,)), dma((ych,))],
            compiler_params=pltpu.CompilerParams(collective_id=1, has_side_effects=True, vmem_limit_bytes=8 * MIB),
        )(part, pltpu.with_memory_space_constraint(wo, pltpu.HBM))
        shape = (nb, npos, nkv, dh)
        return y, ko.reshape(shape), vo.reshape(shape)

    cache = P('dp', 'sp', None, None)
    return jax.shard_map(
        local, mesh=mesh,
        in_specs=(P('dp', None), P(None, None), P(None, None), P(None, None), P('sp', None),
                  cache, cache, P('dp'), P('dp')),
        out_specs=(P('dp', None), cache, cache),
        check_vma=False)
```

```python
import functools

import jax
import jax.numpy as jnp
from jax import lax
from jax.experimental import pallas as pl
from jax.experimental.pallas import tpu as pltpu
from jax.sharding import PartitionSpec as P

MESH = pl.DeviceIdType.MESH
ANY = pl.BlockSpec(memory_space=pl.ANY)
VMEM = pl.BlockSpec(memory_space=pltpu.VMEM)
SMEM = pl.BlockSpec(memory_space=pltpu.SMEM)
f32 = jnp.float32
bf16 = jnp.bfloat16
LOG2E = 1.4426950408889634
MIB = 1 << 20


def greet(n):
    me = lax.axis_index('sp')
    barrier = pltpu.get_barrier_semaphore()
    for d in range(1, n):
        pl.semaphore_signal(barrier, inc=1, device_id={'sp': lax.rem(me + d, n)}, device_id_type=MESH)


def awaited(n):
    pl.semaphore_wait(pltpu.get_barrier_semaphore(), n - 1)


def lookup(n, wch, ch, wide, slabs, early, kpre, pos_hbm, lens_hbm, x, wq, wk, wv, kc, vc, gat_out, kbuf, vbuf, sc, mrun, snew, qbd,
           pos, lens, xb, wqb, wab, send, gat, isem, xsem, wsem, ksem, vsem, ssem, rsem):
    me = lax.axis_index('sp')
    nb, dm = xb.shape
    dq, dh, da = wqb.shape[1], gat.shape[3], wab.shape[1]
    rows = dm // wch
    g = dq // dh
    nkv = n
    npos = kbuf.shape[1] // nkv
    nch = npos // ch
    total = nb * nch
    crow = ch * nkv
    srow = crow // slabs
    heads = 128 // slabs
    start = me * npos
    ninf = -jnp.inf

    def chunk(i):
        return i // nch, pl.ds(pl.multiple_of(i % nch * crow, crow), crow)

    def read_k(i):
        b, r = chunk(i)
        return pltpu.make_async_copy(kc.at[b, r], kbuf.at[b, r], ksem.at[i])

    def read_v(i):
        b, r = chunk(i)
        return pltpu.make_async_copy(vc.at[b, r], vbuf.at[b, r], vsem.at[i])

    xcp = pltpu.make_async_copy(x, xb, xsem)
    xcp.start()
    icps = [pltpu.make_async_copy(pos_hbm, pos, isem.at[0]), pltpu.make_async_copy(lens_hbm, lens, isem.at[1])]
    for cp in icps:
        cp.start()
    even = lax.rem(me, 2) == 0

    def read_q(c):
        r = pl.ds(c * rows, rows)
        return pltpu.make_async_copy(wq.at[r, pl.ds(pl.multiple_of(me * dq, 128), dq)], wqb.at[r], wsem.at[0, c])

    def read_a(w, c):
        r = pl.ds(c * rows, rows)
        return pltpu.make_async_copy(w.at[r, pl.ds(pl.multiple_of(me // 2 * da, 128), da)], wab.at[r], wsem.at[1, c])

    for c in range(wch):
        read_q(c).start()

    @pl.when(even)
    def _():
        for c in range(wch):
            read_a(wk, c).start()

    @pl.when(jnp.logical_not(even))
    def _():
        for c in range(wch):
            read_a(wv, c).start()

    for i in range(kpre):
        read_k(i).start()
    greet(n)
    xcp.wait()
    aq = jnp.zeros((nb, dq), f32)
    aa = jnp.zeros((nb, da), f32)
    for c in range(wch):
        read_q(c).wait()
        read_a(wk, c).wait()
        for i in range(kpre + c * (total - kpre) // wch, kpre + (c + 1) * (total - kpre) // wch):
            read_k(i).start()
        xc = xb[:, c * rows:(c + 1) * rows]
        r = pl.ds(c * rows, rows)
        aq += jnp.dot(xc, wqb[r, :], preferred_element_type=f32)
        aa += jnp.dot(xc, wab[r, :], preferred_element_type=f32)
    for b in range(nb):
        pieces = [aq[b:b + 1, i * dh:(i + 1) * dh] for i in range(g)] + [aa[b:b + 1, i * dh:(i + 1) * dh] for i in range(2)]
        pieces.append(jnp.zeros((8 - g - 2, dh), f32))
        tile = jnp.concatenate(pieces, axis=0).astype(bf16)
        send[b] = tile
        gat[me, b] = tile
    for i in range(early):
        read_v(i).start()
    awaited(n)
    out = []
    for d in range(1, n):
        cp = pltpu.make_async_remote_copy(
            src_ref=send, dst_ref=gat.at[me], send_sem=ssem.at[d], recv_sem=rsem.at[d],
            device_id={'sp': lax.rem(me + d, n)}, device_id_type=MESH)
        cp.start()
        out.append(cp)
    for cp in out:
        cp.wait()

    for cp in icps:
        cp.wait()
    gat_out[...] = gat[...]
    gf = gat[...].astype(f32)
    sub = lax.broadcasted_iota(jnp.int32, (nkv, 128), 0)
    lane = lax.broadcasted_iota(jnp.int32, (nkv, 128), 1)
    own = sub == (lane % heads) // g
    wrow = wide * nkv // slabs
    wch_n = npos // wide
    per = wide // ch
    first = jnp.where(own, lane // heads * (wide // slabs), 1 << 29)
    for b in range(nb):
        q = jnp.concatenate([gf[i, b, 0:g] for i in range(nkv)], axis=0)
        kn = jnp.concatenate([gf[i // 2 * 2, b, g + i % 2:g + i % 2 + 1] for i in range(nkv)], axis=0)
        zero = jnp.zeros_like(q)
        for s in range(slabs):
            a = jnp.concatenate([q if i == s else zero for i in range(slabs)], axis=0)
            qbd[b, s * dh:(s + 1) * dh, :] = a.T.astype(bf16)
        k16 = jnp.concatenate([kn, jnp.zeros_like(kn)], axis=0).astype(bf16)
        t = jnp.dot(k16, qbd[b, 0:dh, :], preferred_element_type=f32)[0:nkv]
        here = jnp.logical_and(pos[b] >= start, pos[b] < jnp.minimum(start + npos, lens[b]))
        limit = jnp.where(here, heads, 0)
        t = jnp.where(jnp.logical_and(own, lane < limit), t, ninf)
        snew[b] = t
        mrun[b] = t

    def scores(c, _):
        b = 0
        for t in range(per):
            read_k(c * per + t).wait()

        @pl.when(c * per + early < total)
        def _():
            for t in range(per):
                read_v(c * per + t + early).start()

        lim = jnp.minimum(pos[b], lens[b]) - start - c * wide
        acc = None
        for s in range(0, slabs, 2):
            k2 = jnp.concatenate(
                [kbuf[b, pl.ds(pl.multiple_of((c * slabs + s + t) * wrow, wrow), wrow), :] for t in range(2)], axis=1)
            t = jnp.dot(k2, qbd[b, s * dh:(s + 2) * dh, :], preferred_element_type=f32)
            acc = t if acc is None else acc + t
        acc = acc.reshape(wrow // nkv, nkv, 128)
        left = lim - lax.broadcasted_iota(jnp.int32, acc.shape, 0)
        t = jnp.where(first[None] < left, acc, ninf)
        sc[pl.ds(pl.multiple_of(c * wrow, wrow), wrow), :] = t.reshape(wrow, 128)
        mrun[b] = jnp.maximum(mrun[b], t.max(0))
        return 0

    lax.fori_loop(0, wch_n, scores, 0)
    for i in range(nch, total):
        read_k(i).wait()

    def landed(i, _):
        read_v(i).wait()
        return 0

    lax.fori_loop(0, total, landed, 0)


def attend(ch, wide, slabs, pos_hbm, lens_hbm, gat, kbuf, vbuf, sc, mrun, snew, qbd, part, ko, vo, pos, lens, rest, mall, lrun, orun, knew, vnew,
           isem, ksem, vsem, nsem):
    me = lax.axis_index('sp')
    nkv, nb, _, dh = gat.shape
    npos = kbuf.shape[1] // nkv
    nch = npos // ch
    total = nb * nch
    crow = ch * nkv
    srow = crow // slabs
    heads = 128 // slabs
    g = heads // nkv
    start = me * npos
    scale = dh ** -0.5 * LOG2E
    ninf = -jnp.inf

    icps = [pltpu.make_async_copy(pos_hbm, pos, isem.at[0]), pltpu.make_async_copy(lens_hbm, lens, isem.at[1])]
    for cp in icps:
        cp.start()

    def writes(i):
        b, r = i // nch, pl.ds(pl.multiple_of(i % nch * crow, crow), crow)
        return (pltpu.make_async_copy(kbuf.at[b, r], ko.at[b, r], ksem.at[i]),
                pltpu.make_async_copy(vbuf.at[b, r], vo.at[b, r], vsem.at[i]))

    def begin(i, _):
        for t, cp in enumerate(writes(i)):
            cp.start(priority=t)
        return 0

    lax.fori_loop(0, total, begin, 0)

    gf = gat[...].astype(f32)
    lrun[...] = jnp.zeros_like(lrun)
    orun[...] = jnp.zeros_like(orun)
    for b in range(nb):
        knew[b] = jnp.concatenate([gf[i // 2 * 2, b, g + i % 2:g + i % 2 + 1] for i in range(nkv)], axis=0).astype(bf16)
        vnew[b] = jnp.concatenate([gf[i // 2 * 2 + 1, b, g + i % 2:g + i % 2 + 1] for i in range(nkv)], axis=0).astype(bf16)
        mall[b] = mrun[b]

    wrow = wide * nkv // slabs
    wch_n = npos // wide

    sub = lax.broadcasted_iota(jnp.int32, (nkv, 128), 0)
    lane = lax.broadcasted_iota(jnp.int32, (nkv, 128), 1)
    own = sub == (lane % heads) // g
    first = jnp.where(own, lane // heads * (wide // slabs), 1 << 29)

    def settle(b):
        m = jnp.broadcast_to(mall[b].max(0, keepdims=True), (nkv, 128))
        k = heads
        while k < 128:
            m = jnp.maximum(m, pltpu.roll(m, k, 1))
            k *= 2
        mall[b] = m

    def mix(b, scored, c):
        lim = jnp.minimum(pos[b], lens[b]) - start - c * wide

        @pl.when(lim > 0)
        def _():
            m = mall[b]
            m = jnp.where(m == ninf, 0.0, m)
            t = scored[pl.ds(pl.multiple_of(c * wrow, wrow), wrow), :].reshape(wrow // nkv, nkv, 128)
            e = jnp.exp2((t - m[None]) * scale)
            lrun[b] += e.sum(0)
            et = e.reshape(wrow, 128).astype(bf16).T
            o = orun[b]
            for s in range(slabs):
                v = vbuf[b, pl.ds(pl.multiple_of((c * slabs + s) * wrow, wrow), wrow), :]
                o += jnp.dot(et[s * heads:(s + 1) * heads], v, preferred_element_type=f32)
            orun[b] = o

    def scores(b, scored, c):
        lim = jnp.minimum(pos[b], lens[b]) - start - c * wide

        @pl.when(lim > 0)
        def _():
            acc = None
            for s in range(0, slabs, 2):
                k2 = jnp.concatenate(
                    [kbuf[b, pl.ds(pl.multiple_of((c * slabs + s + t) * wrow, wrow), wrow), :] for t in range(2)], axis=1)
                t = jnp.dot(k2, qbd[b, s * dh:(s + 2) * dh, :], preferred_element_type=f32)
                acc = t if acc is None else acc + t
            acc = acc.reshape(wrow // nkv, nkv, 128)
            left = lim - lax.broadcasted_iota(jnp.int32, acc.shape, 0)
            t = jnp.where(first[None] < left, acc, ninf)
            scored[pl.ds(pl.multiple_of(c * wrow, wrow), wrow), :] = t.reshape(wrow, 128)
            mall[b] = jnp.maximum(mall[b], t.max(0))

    def loop(step, b, scored):
        def body(c, _):
            step(b, scored, c)
            return 0

        lax.fori_loop(0, wch_n, body, 0)

    for cp in icps:
        cp.wait()
    settle(0)
    loop(mix, 0, sc)
    for b in range(1, nb):
        loop(scores, b, rest)
        settle(b)
        loop(mix, b, rest)

    half = lax.broadcasted_iota(jnp.int32, (heads, 128), 1) < 64
    for b in range(nb):
        m = mall[b]
        e = jnp.exp2((snew[b] - jnp.where(m == ninf, 0.0, m)) * scale)
        pad = jnp.zeros_like(e)
        e16 = jnp.concatenate([e, pad], axis=0).astype(bf16)
        v16 = jnp.concatenate([vnew[b].astype(f32), pad], axis=0).astype(bf16)
        o = orun[b] + lax.dot_general(e16, v16, (((0,), (0,)), ((), ())), preferred_element_type=f32)[0:heads]
        l = jnp.broadcast_to((lrun[b] + e).sum(0, keepdims=True), (nkv, 128))
        k = heads
        while k < 128:
            l = l + pltpu.roll(l, k, 1)
            k *= 2
        lt = jnp.broadcast_to(l[0:1], (128, 128)).T[0:heads]
        mt = jnp.broadcast_to(m[0:1] * scale, (128, 128)).T[0:heads]
        ml = jnp.where(half, mt, lt)
        for i in range(nkv):
            part[i, 0, b * g:(b + 1) * g, :] = o[i * g:(i + 1) * g, :]
            part[i, 1, b * g:(b + 1) * g, :] = ml[i * g:(i + 1) * g, :]

    def rows(b):
        r = pl.ds(pl.multiple_of((pos[b] - start) * nkv, nkv), nkv)
        return (pltpu.make_async_copy(knew.at[b], ko.at[b, r], nsem.at[b, 0]),
                pltpu.make_async_copy(vnew.at[b], vo.at[b, r], nsem.at[b, 1]))

    def written(i, _):
        for cp in writes(i):
            cp.wait()
        b = i // nch
        p = pos[b] - start - i % nch * ch

        @pl.when(jnp.logical_and(p >= 0, p < ch))
        def _():
            for cp in rows(b):
                cp.start()

        return 0

    lax.fori_loop(0, total, written, 0)
    for b in range(nb):
        p = pos[b] - start

        @pl.when(jnp.logical_and(p >= 0, p < npos))
        def _():
            for cp in rows(b):
                cp.wait()


def combine(n, nb, ych, part, wo, y, wob, rbuf, xs, mine, far, half, twin, wsem, ssem, rsem, ysem, zsem, hsem, tsem):
    me = lax.axis_index('sp')
    cols = wo.shape[1] // ych
    cps = []
    for c in range(ych):
        cp = pltpu.make_async_copy(wo.at[:, pl.ds(c * cols, cols)], wob.at[c], wsem.at[c])
        cp.start()
        cps.append(cp)
    greet(n)
    awaited(n)
    out = []
    for d in range(1, n):
        peer = lax.rem(me + d, n)
        cp = pltpu.make_async_remote_copy(
            src_ref=part.at[peer], dst_ref=rbuf.at[me], send_sem=ssem.at[d], recv_sem=rsem.at[d],
            device_id={'sp': peer}, device_id_type=MESH)
        cp.start()
        out.append(cp)
    rbuf[me] = part[me]
    for cp in out:
        cp.wait()
    o = rbuf[:, 0]
    ml = rbuf[:, 1]
    m = jnp.broadcast_to(ml[:, :, 0:1], o.shape)
    l = jnp.broadcast_to(ml[:, :, 64:65], o.shape)
    a = jnp.exp2(m - m.max(0)[None])
    out8 = (a * o).sum(0) / (a * l).sum(0)
    g = out8.shape[0] // nb
    dh = out8.shape[1]
    xs[...] = jnp.zeros_like(xs)
    for b in range(nb):
        for j in range(g):
            xs[b:b + 1, j * dh:(j + 1) * dh] = out8[b * g + j:b * g + j + 1]
    xl = xs[...].astype(bf16)
    over_x = me + 2 - 4 * lax.rem(me // 2, 2)
    over_y = me + 4 - 8 * (me // 4)
    sent = []
    for c in range(ych):
        cps[c].wait()
        mine[c] = jnp.dot(xl, wob[c], preferred_element_type=f32)[0:nb]
        for j, peer in enumerate((over_x, over_y, over_x + over_y - me)):
            cp = pltpu.make_async_remote_copy(
                src_ref=mine.at[c], dst_ref=far.at[j, c], send_sem=ysem.at[c, j], recv_sem=zsem.at[c, j],
                device_id={'sp': peer}, device_id_type=MESH)
            cp.start()
            sent.append(cp)
    swaps = []
    for c in range(ych):
        for j in range(3):
            sent[3 * c + j].wait()
        half[c] = (mine[c] + far[0, c]) + (far[1, c] + far[2, c])
        cp = pltpu.make_async_remote_copy(
            src_ref=half.at[c], dst_ref=twin.at[c], send_sem=hsem.at[c], recv_sem=tsem.at[c],
            device_id={'sp': me + 1 - 2 * lax.rem(me, 2)}, device_id_type=MESH)
        cp.start()
        swaps.append(cp)
    for c in range(ych):
        swaps[c].wait()
        y[:, c * cols:(c + 1) * cols] = (half[c] + twin[c]).astype(bf16)


def solution(mesh):
    n = mesh.shape['sp']

    def local(x, wq, wk, wv, wo, kc, vc, pos, lens):
        nb, npos, nkv, dh = kc.shape
        dm = x.shape[1]
        dq = wq.shape[1] // n
        dma = pltpu.SemaphoreType.DMA
        kc = kc.reshape(nb, npos * nkv, dh)
        vc = vc.reshape(nb, npos * nkv, dh)
        wch, ch, wide, slabs, early, kpre = 4, 1024, 1024, 4, 4, 1
        nch = npos // ch
        small = jax.ShapeDtypeStruct((nb, nkv, 128), f32)
        gat, kbuf, vbuf, sc, mrun, snew, qbd = pl.pallas_call(
            functools.partial(lookup, n, wch, ch, wide, slabs, early, kpre),
            name='lookup',
            out_shape=(jax.ShapeDtypeStruct((n, nb, 8, dh), bf16), pltpu.VMEM(kc.shape, bf16), pltpu.VMEM(vc.shape, bf16),
                       pltpu.VMEM((npos * nkv // slabs, 128), f32), small, small,
                       jax.ShapeDtypeStruct((nb, slabs * dh, 128), bf16)),
            in_specs=[ANY] * 8,
            out_specs=(VMEM,) * 7,
            scratch_shapes=[
                pltpu.SMEM((nb,), jnp.int32), pltpu.SMEM((nb,), jnp.int32),
                pltpu.VMEM(x.shape, bf16), pltpu.VMEM((dm, dq), bf16), pltpu.VMEM((dm, 2 * dh), bf16),
                pltpu.VMEM((nb, 8, dh), bf16), pltpu.VMEM((n, nb, 8, dh), bf16),
                dma((2,)), dma, dma((2, wch)), dma((nb * nch,)), dma((nb * nch,)), dma((n,)), dma((n,))],
            compiler_params=pltpu.CompilerParams(collective_id=0, has_side_effects=True, vmem_limit_bytes=12 * MIB),
        )(*(pltpu.with_memory_space_constraint(t, pltpu.HBM) for t in (pos, lens, x, wq, wk, wv, kc, vc)))

        part, ko, vo = pl.pallas_call(
            functools.partial(attend, 2 * ch, wide, slabs),
            name='attend',
            out_shape=(jax.ShapeDtypeStruct((n, 2, 8, dh), f32), pltpu.HBM(kc.shape, bf16), pltpu.HBM(vc.shape, bf16)),
            in_specs=[ANY] * 2 + [VMEM] * 7,
            out_specs=(VMEM, ANY, ANY),
            scratch_shapes=[
                pltpu.SMEM((nb,), jnp.int32), pltpu.SMEM((nb,), jnp.int32), pltpu.VMEM((npos * nkv // slabs, 128), f32),
                pltpu.VMEM((nb, nkv, 128), f32), pltpu.VMEM((nb, nkv, 128), f32), pltpu.VMEM((nb, 128 // slabs, dh), f32),
                pltpu.VMEM((nb, nkv, dh), bf16), pltpu.VMEM((nb, nkv, dh), bf16),
                dma((2,)), dma((nb * nch,)), dma((nb * nch,)), dma((nb, 2))],
            compiler_params=pltpu.CompilerParams(vmem_limit_bytes=12 * MIB),
        )(*(pltpu.with_memory_space_constraint(t, pltpu.HBM) for t in (pos, lens)), gat, kbuf, vbuf, sc, mrun, snew, qbd)

        ych = 4
        cols = wo.shape[1] // ych
        y = pl.pallas_call(
            functools.partial(combine, n, nb, ych),
            name='combine',
            out_shape=jax.ShapeDtypeStruct((nb, wo.shape[1]), bf16),
            in_specs=[VMEM, ANY],
            out_specs=VMEM,
            scratch_shapes=[
                pltpu.VMEM((ych, wo.shape[0], cols), bf16), pltpu.VMEM((n, 2, 8, dh), f32), pltpu.VMEM((8, wo.shape[0]), f32),
                pltpu.VMEM((ych, nb, cols), f32), pltpu.VMEM((3, ych, nb, cols), f32),
                pltpu.VMEM((ych, nb, cols), f32), pltpu.VMEM((ych, nb, cols), f32),
                dma((ych,)), dma((n,)), dma((n,)), dma((ych, 3)), dma((ych, 3)), dma((ych,)), dma((ych,))],
            compiler_params=pltpu.CompilerParams(collective_id=1, has_side_effects=True, vmem_limit_bytes=8 * MIB),
        )(part, pltpu.with_memory_space_constraint(wo, pltpu.HBM))
        shape = (nb, npos, nkv, dh)
        return y, ko.reshape(shape), vo.reshape(shape)

    cache = P('dp', 'sp', None, None)
    return jax.shard_map(
        local, mesh=mesh,
        in_specs=(P('dp', None), P(None, None), P(None, None), P(None, None), P('sp', None),
                  cache, cache, P('dp'), P('dp')),
        out_specs=(P('dp', None), cache, cache),
        check_vma=False)
```
